128 devices in a mesh: py: 8 (over z, x_hi), px: 4 (over y_hi, core), pz: 4 (over y_lo, x_lo).
Axes of the slice: x: 4 (x_hi: 2, x_lo: 2; x = x_hi * 2 + x_lo), y: 4 (y_hi: 2, y_lo: 2; y = y_hi * 2 + y_lo), z: 4, core: 2. Of those that a mesh axis runs over, the one named last changes fastest.
Arguments:
- initial_density: float32 [32, 256, 384, 128], P('py', 'px', 'pz'), may hold values from 0.2 to 1.8
- inverse_limit: float32 [32, 256, 384, 128], P('py', 'px', 'pz'), may hold values from 0.5 to 2
Outputs:
- temperature_end: float32 [32, 256, 384, 128], P('py', 'px', 'pz')
The draws below stay inside these ranges and needn't reach their ends.
All inputs are finite; a program needn't handle non-finite values.
Results may differ from the reference program's by a relative error of at most 0.00002.
Values sent between devices are 32-bit elements; how exact they have to be, the bound alone decides.
No kernel may reach another device: no remote copies, remote signals or barrier semaphores. Data moves between devices by JAX's collectives and lax.ppermute only.
A program may use at most 384 MiB of HBM per device.

```python
import jax
import jax.numpy as jnp
from jax import lax

WIDTH_SECOND = 32
WIDTH_FIRST = 256
WIDTH_THIRD = 384
DEPTH_TOTAL = 128
STEPS = 3


def shard_levels(rng, shape, cuts, low, top_value):
    loudness = 1.0
    for position, shards_of in cuts:
        heights = jax.random.uniform(jax.random.fold_in(jax.random.fold_in(rng, 6), position), (shards_of,), jnp.float32, low / len(cuts), top_value / len(cuts))
        loudness = loudness * jnp.repeat(jnp.exp(heights), shape[position] // shards_of).reshape((-1,) + (1,) * (len(shape) - 1 - position))
    return loudness


def setup_inputs(seed: int = 0) -> dict:
    streams_of = jax.random.split(jax.random.key(seed), 3)
    return {
        "initial_density": jnp.clip(0.2 + 1.5999999 * jax.random.uniform(streams_of[0], (WIDTH_SECOND, WIDTH_FIRST, WIDTH_THIRD, DEPTH_TOTAL), jnp.float32) ** shard_levels(streams_of[0], (WIDTH_SECOND, WIDTH_FIRST, WIDTH_THIRD, DEPTH_TOTAL), ((0, 8), (1, 4), (2, 4)), -0.2, 0.2), 0.2, 1.8),
        "inverse_limit": jnp.clip(0.5 + 1.5 * jax.random.uniform(streams_of[1], (WIDTH_SECOND, WIDTH_FIRST, WIDTH_THIRD, DEPTH_TOTAL), jnp.float32) ** shard_levels(streams_of[1], (WIDTH_SECOND, WIDTH_FIRST, WIDTH_THIRD, DEPTH_TOTAL), ((0, 8), (1, 4), (2, 4)), -0.2, 0.2), 0.5, 2.0),
    }


def inner_cells(values, dims):
    for dim in dims:
        values = lax.slice_in_dim(values, 1, values.shape[dim] - 1, axis=dim)
    return values


def boundary_cells(values, dim, start, dims):
    remaining_parts = [other for other in dims if other != dim]
    values = inner_cells(values, remaining_parts)
    return lax.slice_in_dim(values, start, start + values.shape[dim] - 2, axis=dim)


def advance_population(haloed_population, inverse_limit):
    middle = inner_cells(haloed_population, (0, 1, 2))
    lower = [boundary_cells(haloed_population, dim, 0, (0, 1, 2)) for dim in (0, 1, 2)]
    upper = [boundary_cells(haloed_population, dim, 2, (0, 1, 2)) for dim in (0, 1, 2)]
    spread = lower[0] + upper[0] + lower[1] + upper[1] + lower[2] + upper[2] - 6.0 * middle
    return middle + 0.1 * spread + 0.2 * middle * (1.0 - middle * inverse_limit)


def reference(initial_density, inverse_limit):
    for step in range(STEPS):
        initial_density = advance_population(jnp.pad(initial_density, ((1, 1), (1, 1), (1, 1), (0, 0)), mode="constant"), inverse_limit)
    return initial_density
```

```python
import functools

import jax
import jax.numpy as jnp
from jax import lax
from jax.experimental import pallas as pl
from jax.experimental.pallas import tpu as pltpu
from jax.sharding import PartitionSpec as P


STEPS = 3
ROWS = 8
TILE = 16
DIRECT = 48

EVEN_CUTS = [(0, 1), (1, 0), (2, 3), (3, 2), (4, 5), (5, 4), (6, 7), (7, 6)]
ODD_CUTS = [(1, 2), (2, 1), (3, 4), (4, 3), (5, 6), (6, 5)]
RELAYS = [
    ([(2, 0), (5, 7)], [(0, 1), (7, 6)]),
    ([(4, 0), (3, 7)], [(0, 3), (7, 4)]),
    ([(6, 0), (1, 7)], [(0, 5), (7, 2)]),
]
VMEM = 20 * 1024 * 1024


def struct(*shape):
    return jax.ShapeDtypeStruct(shape, jnp.float32)


def fixed(*shape):
    return pl.BlockSpec(shape, lambda i, *_: (0,) * len(shape))


def partial_kernel(first, last, odd_ref, *refs):
    planes = [refs[3 * s : 3 * s + 3] for s in range(4)]
    inverse, px_low, px_high, pz_low, pz_high = refs[12:17]
    part_o, part_e, kept, mx_low, mx_high, mz_low, mz_high = (refs[17:] + (None,) * 4)[:7]
    i, blocks = pl.program_id(0), pl.num_programs(0)
    odd = odd_ref[0]
    shape = px_low.shape[1:]
    depth = shape[0]
    z = lax.broadcasted_iota(jnp.int32, shape, 0)

    def stored(s):
        return jnp.where(odd == 1, 3 - s, s)

    def edge(s):
        return stored(s) if first else s

    def main(s, r):
        ref = planes[s][0]
        return ref[r] if len(ref.shape) == 3 else ref[0, r]

    def one_row(r, before, after):
        for s in range(4):
            c = main(s, r)
            below = jnp.where(z == 0, pz_low[edge(s), pl.ds(r, 1), :], pltpu.roll(c, 1, 0))
            above = jnp.where(z == depth - 1, pz_high[edge(s), pl.ds(r, 1), :], pltpu.roll(c, depth - 1, 0))
            total = (before(s) + after(s)) + (below + above)
            if s > 0:
                total = total + main(s - 1, r)
            if s < 3:
                total = total + main(s + 1, r)
            value = c * (0.6 - 0.2 * c * inverse[stored(s), r]) + 0.1 * total
            if s == 0:
                part_o[r] = value
            elif s == 3:
                part_e[r] = value
            elif last:
                kept[stored(s), r] = value
            else:
                kept[s - 1, r] = value
                mz_low[s - 1, pl.ds(r, 1), :] = value[0:1, :]
                mz_high[s - 1, pl.ds(r, 1), :] = value[depth - 1 : depth, :]

    def earlier(s):
        return jnp.where(i == 0, px_low[edge(s)], planes[s][1][...].reshape(shape))

    def later(s):
        return jnp.where(i == blocks - 1, px_high[edge(s)], planes[s][2][...].reshape(shape))

    one_row(0, earlier, lambda s: main(s, 1))

    @pl.loop(1, ROWS - 1)
    def _(r):
        one_row(r, lambda s: main(s, r - 1), lambda s: main(s, r + 1))

    one_row(ROWS - 1, lambda s: main(s, ROWS - 2), later)
    if not last:

        @pl.when(i == 0)
        def _():
            mx_low[...] = kept[:, 0]

        @pl.when(i == blocks - 1)
        def _():
            mx_high[...] = kept[:, ROWS - 1]


def partial_step(step, odd, o, mid, e, inverse, px, pz):
    first, last = step == 0, step == STEPS - 1
    rows, depth, levels = o.shape

    def specs(plane):
        if plane is None:
            shape, at = (lambda k: (k, depth, levels)), (lambda j, odd_ref: (j, 0, 0))
        else:
            shape, at = (lambda k: (1, k, depth, levels)), (lambda j, odd_ref: (plane(odd_ref), j, 0, 0))
        return [
            pl.BlockSpec(shape(ROWS), lambda i, odd_ref: at(i, odd_ref)),
            pl.BlockSpec(shape(1), lambda i, odd_ref: at(jnp.maximum(i * ROWS - 1, 0), odd_ref)),
            pl.BlockSpec(shape(1), lambda i, odd_ref: at(jnp.minimum(i * ROWS + ROWS, rows - 1), odd_ref)),
        ]

    def middle(s):
        if first:
            return lambda odd_ref: jnp.where(odd_ref[0] == 1, 3 - s, s)
        return lambda odd_ref: s - 1

    def block(planes):
        return pl.BlockSpec((planes, ROWS, depth, levels), lambda i, odd_ref: (0, i, 0, 0))

    def ends(planes):
        return pl.BlockSpec((planes, ROWS, levels), lambda i, odd_ref: (0, i, 0))

    face = pl.BlockSpec((ROWS, depth, levels), lambda i, odd_ref: (i, 0, 0))
    out_specs = [face, face, block(4 if last else 2)]
    out_shape = [struct(*o.shape), struct(*o.shape), struct(4 if last else 2, *o.shape)]
    if not last:
        out_specs += [fixed(2, depth, levels)] * 2 + [ends(2)] * 2
        out_shape += [struct(2, depth, levels)] * 2 + [struct(2, rows, levels)] * 2
    return pl.pallas_call(
        functools.partial(partial_kernel, first, last),
        grid_spec=pltpu.PrefetchScalarGridSpec(
            num_scalar_prefetch=1,
            grid=(rows // ROWS,),
            in_specs=specs(None)
            + specs(middle(1))
            + specs(middle(2))
            + specs(None)
            + [block(4), fixed(4, depth, levels), fixed(4, depth, levels), ends(4), ends(4)],
            out_specs=out_specs,
        ),
        out_shape=out_shape,
        compiler_params=pltpu.CompilerParams(vmem_limit_bytes=VMEM),
        cost_estimate=pl.CostEstimate(flops=60_000_000, bytes_accessed=40_000_000, transcendentals=0),
        name="partial_step",
    )(odd, *([o] * 3), *([mid] * 6), *([e] * 3), inverse, *px, *pz)


def finish_even_kernel(part, halo, face, x_ends, z_ends):
    i, blocks = pl.program_id(0), pl.num_programs(0)
    depth = face.shape[1]
    face[...] = part[...] + 0.1 * halo[...]
    z_ends[0] = face[:, 0, :]
    z_ends[1] = face[:, depth - 1, :]

    @pl.when(i == 0)
    def _():
        x_ends[0] = face[0]

    @pl.when(i == blocks - 1)
    def _():
        x_ends[1] = face[TILE - 1]


def finish_even(part, halo):
    rows, depth, levels = part.shape
    face = pl.BlockSpec((TILE, depth, levels), lambda i: (i, 0, 0))
    return pl.pallas_call(
        finish_even_kernel,
        grid=(rows // TILE,),
        in_specs=[face, face],
        out_specs=[face, fixed(2, depth, levels), pl.BlockSpec((2, TILE, levels), lambda i: (0, i, 0))],
        out_shape=[struct(*part.shape), struct(2, depth, levels), struct(2, rows, levels)],
        compiler_params=pltpu.CompilerParams(vmem_limit_bytes=VMEM),
        cost_estimate=pl.CostEstimate(flops=6_000_000, bytes_accessed=9_500_000, transcendentals=0),
        name="finish_even",
    )(part, halo)


def odd_halo(i, halo, relayed, store):
    straight = DIRECT // TILE

    @pl.when(i < straight)
    def _():
        store(halo[...])

    @pl.when(i >= straight)
    def _():
        store(relayed[0][...] + relayed[1][...] + relayed[2][...])


def odd_halo_specs(depth, levels):
    straight = DIRECT // TILE
    top = pl.BlockSpec((TILE, depth, levels), lambda i, *_: (jnp.minimum(i, straight - 1), 0, 0))
    rest = pl.BlockSpec((TILE, depth, levels), lambda i, *_: (jnp.maximum(i - straight, 0), 0, 0))
    return top, rest


def finish_odd_kernel(part, halo, r0, r1, r2, mx_low, mx_high, mz_low, mz_high, ex, ez, *outs):
    face, top, rest, x_low, x_high, z_low, z_high = outs
    i, blocks = pl.program_id(0), pl.num_programs(0)
    depth = face.shape[1]

    def store(h):
        face[...] = part[...] + 0.1 * h

    odd_halo(i, halo, (r0, r1, r2), store)

    @pl.when(i < DIRECT // TILE)
    def _():
        top[...] = face[...]

    @pl.when(i >= DIRECT // TILE)
    def _():
        rest[...] = face[...]

    for z_out, z_mid, k, at in ((z_low, mz_low, 0, 0), (z_high, mz_high, 1, depth - 1)):
        z_out[0] = face[:, at, :]
        z_out[1:3] = z_mid[...]
        z_out[3] = ez[k]

    @pl.when(i == 0)
    def _():
        x_low[0] = face[0]
        x_low[1:3] = mx_low[...]
        x_low[3] = ex[0]

    @pl.when(i == blocks - 1)
    def _():
        x_high[0] = face[TILE - 1]
        x_high[1:3] = mx_high[...]
        x_high[3] = ex[1]


def finish_odd(part, halo, relayed, mids, ex, ez):
    rows, depth, levels = part.shape
    face = pl.BlockSpec((TILE, depth, levels), lambda i: (i, 0, 0))
    top, rest = odd_halo_specs(depth, levels)

    def ends(planes):
        return pl.BlockSpec((planes, TILE, levels), lambda i: (0, i, 0))

    x2, x4 = fixed(2, depth, levels), fixed(4, depth, levels)
    return pl.pallas_call(
        finish_odd_kernel,
        grid=(rows // TILE,),
        in_specs=[face, top, rest, rest, rest, x2, x2, ends(2), ends(2), x2, ends(2)],
        out_specs=[face, top, rest, x4, x4, ends(4), ends(4)],
        out_shape=[struct(*part.shape), struct(DIRECT, depth, levels), struct(rows - DIRECT, depth, levels)]
        + [struct(4, depth, levels)] * 2
        + [struct(4, rows, levels)] * 2,
        compiler_params=pltpu.CompilerParams(vmem_limit_bytes=VMEM),
        cost_estimate=pl.CostEstimate(flops=6_000_000, bytes_accessed=12_600_000, transcendentals=0),
        name="finish_odd",
    )(part, halo, *relayed, *mids, ex, ez)


def place_even_kernel(at_ref, part, halo, whole, out):
    out[0] = part[...] + 0.1 * halo[...]


def place_odd_kernel(at_ref, part, halo, r0, r1, r2, whole, out):
    def store(h):
        out[0] = part[...] + 0.1 * h

    odd_halo(pl.program_id(0), halo, (r0, r1, r2), store)


def place(kernel, at, part, halos, whole, specs):
    rows, depth, levels = part.shape
    face = pl.BlockSpec((TILE, depth, levels), lambda i, at_ref: (i, 0, 0))
    return pl.pallas_call(
        kernel,
        grid_spec=pltpu.PrefetchScalarGridSpec(
            num_scalar_prefetch=1,
            grid=(rows // TILE,),
            in_specs=[face, *(specs or [face]), pl.BlockSpec(memory_space=pl.ANY)],
            out_specs=pl.BlockSpec((1, TILE, depth, levels), lambda i, at_ref: (at_ref[0], i, 0, 0)),
        ),
        out_shape=struct(*whole.shape),
        input_output_aliases={2 + len(halos): 0},
        compiler_params=pltpu.CompilerParams(vmem_limit_bytes=VMEM),
        cost_estimate=pl.CostEstimate(flops=6_000_000, bytes_accessed=9_500_000, transcendentals=0),
        name="place",
    )(at.astype(jnp.int32).reshape(1), part, *halos, whole)


def local(density, inverse):
    odd = lax.axis_index("py") % 2
    odd_ref = odd.astype(jnp.int32).reshape(1)
    e_plane, o_plane = 3 * (1 - odd), 3 * odd
    e = lax.dynamic_index_in_dim(density, e_plane, 0, keepdims=False)
    o = lax.dynamic_index_in_dim(density, o_plane, 0, keepdims=False)
    mid = density
    rows, depth, levels = o.shape
    top, rest = o[:DIRECT], o[DIRECT:]
    x_low, x_high = density[:, 0], density[:, rows - 1]
    z_low, z_high = density[:, :, 0], density[:, :, depth - 1]
    up = [(k, k + 1) for k in range(3)]
    down = [(b, a) for a, b in up]
    e_halo = lax.ppermute(e, "py", EVEN_CUTS)
    for step in range(STEPS):
        relayed = []
        for to, _ in RELAYS:
            relayed.append(lax.ppermute(rest, "py", to))
        pz = [lax.ppermute(z_high, "pz", up), lax.ppermute(z_low, "pz", down)]
        px = [lax.ppermute(x_high, "px", up), lax.ppermute(x_low, "px", down)]
        o_halo = lax.ppermute(top, "py", ODD_CUTS)
        for k, (_, on) in enumerate(RELAYS):
            relayed[k] = lax.ppermute(relayed[k], "py", on)
        o_part, e_part, mid, *mids = partial_step(step, odd_ref, o, mid, e, inverse, px, pz)
        if step == STEPS - 1:
            break
        e, ex, ez = finish_even(e_part, e_halo)
        e_halo = lax.ppermute(e, "py", EVEN_CUTS)
        o, top, rest, x_low, x_high, z_low, z_high = finish_odd(o_part, o_halo, relayed, mids, ex, ez)
    out = place(place_even_kernel, e_plane, e_part, (e_halo,), mid, None)
    halo, relay = odd_halo_specs(depth, levels)
    return place(place_odd_kernel, o_plane, o_part, (o_halo, *relayed), out, [halo] + [relay] * 3)


def solution(mesh):
    spec = P("py", "px", "pz", None)
    return jax.shard_map(local, mesh=mesh, in_specs=(spec, spec), out_specs=spec, check_vma=False)
```

```python
import functools

import jax
import jax.numpy as jnp
from jax import lax
from jax.experimental import pallas as pl
from jax.experimental.pallas import tpu as pltpu
from jax.sharding import PartitionSpec as P


STEPS = 3
ROWS = 8
TILE = 16
DIRECT = 48

EVEN_CUTS = [(0, 1), (1, 0), (2, 3), (3, 2), (4, 5), (5, 4), (6, 7), (7, 6)]
ODD_CUTS = [(1, 2), (2, 1), (3, 4), (4, 3), (5, 6), (6, 5)]
RELAYS = [
    ([(2, 0), (5, 7)], [(0, 1), (7, 6)]),
    ([(4, 0), (3, 7)], [(0, 3), (7, 4)]),
    ([(6, 0), (1, 7)], [(0, 5), (7, 2)]),
]
VMEM = 20 * 1024 * 1024


def struct(*shape):
    return jax.ShapeDtypeStruct(shape, jnp.float32)


def fixed(*shape):
    return pl.BlockSpec(shape, lambda i, *_: (0,) * len(shape))


def partial_kernel(first, last, odd_ref, *refs):
    planes = [refs[3 * s : 3 * s + 3] for s in range(4)]
    inverse, px_low, px_high, z_even, z_odd, z_on = refs[12:18]
    part_o, part_e, kept, mx_low, mx_high, mz_even, mz_odd = (refs[18:] + (None,) * 4)[:7]
    i, blocks = pl.program_id(0), pl.num_programs(0)
    odd, pz_odd = odd_ref[0], odd_ref[1] == 1
    shape = px_low.shape[1:]
    depth = shape[0]
    z = lax.broadcasted_iota(jnp.int32, shape, 0)

    def stored(s):
        return jnp.where(odd == 1, 3 - s, s)

    def edge(s):
        return stored(s) if first else s

    def main(s, r):
        ref = planes[s][0]
        return ref[r] if len(ref.shape) == 3 else ref[0, r]

    def one_row(r, before, after):
        for s in range(4):
            c = main(s, r)
            over_even, over_odd, over_on = (v[edge(s), pl.ds(r, 1), :] for v in (z_even, z_odd, z_on))
            over_odd = jnp.where(2 * i < blocks, over_odd, over_on)
            below = jnp.where(z == 0, jnp.where(pz_odd, over_even, over_odd), pltpu.roll(c, 1, 0))
            above = jnp.where(z == depth - 1, jnp.where(pz_odd, over_odd, over_even), pltpu.roll(c, depth - 1, 0))
            total = (before(s) + after(s)) + (below + above)
            if s > 0:
                total = total + main(s - 1, r)
            if s < 3:
                total = total + main(s + 1, r)
            value = c * (0.6 - 0.2 * c * inverse[stored(s), r]) + 0.1 * total
            if s == 0:
                part_o[r] = value
            elif s == 3:
                part_e[r] = value
            elif last:
                kept[stored(s), r] = value
            else:
                kept[s - 1, r] = value
                low, high = value[0:1, :], value[depth - 1 : depth, :]
                mz_even[s - 1, pl.ds(r, 1), :] = jnp.where(pz_odd, low, high)
                mz_odd[s - 1, pl.ds(r, 1), :] = jnp.where(pz_odd, high, low)

    def earlier(s):
        return jnp.where(i == 0, px_low[edge(s)], planes[s][1][...].reshape(shape))

    def later(s):
        return jnp.where(i == blocks - 1, px_high[edge(s)], planes[s][2][...].reshape(shape))

    one_row(0, earlier, lambda s: main(s, 1))

    @pl.loop(1, ROWS - 1)
    def _(r):
        one_row(r, lambda s: main(s, r - 1), lambda s: main(s, r + 1))

    one_row(ROWS - 1, lambda s: main(s, ROWS - 2), later)
    if not last:

        @pl.when(i == 0)
        def _():
            mx_low[...] = kept[:, 0]

        @pl.when(i == blocks - 1)
        def _():
            mx_high[...] = kept[:, ROWS - 1]


def partial_step(step, odd, o, mid, e, inverse, halo_ends):
    first, last = step == 0, step == STEPS - 1
    rows, depth, levels = o.shape

    def specs(plane):
        if plane is None:
            shape, at = (lambda k: (k, depth, levels)), (lambda j, odd_ref: (j, 0, 0))
        else:
            shape, at = (lambda k: (1, k, depth, levels)), (lambda j, odd_ref: (plane(odd_ref), j, 0, 0))
        return [
            pl.BlockSpec(shape(ROWS), lambda i, odd_ref: at(i, odd_ref)),
            pl.BlockSpec(shape(1), lambda i, odd_ref: at(jnp.maximum(i * ROWS - 1, 0), odd_ref)),
            pl.BlockSpec(shape(1), lambda i, odd_ref: at(jnp.minimum(i * ROWS + ROWS, rows - 1), odd_ref)),
        ]

    def middle(s):
        if first:
            return lambda odd_ref: jnp.where(odd_ref[0] == 1, 3 - s, s)
        return lambda odd_ref: s - 1

    def block(planes):
        return pl.BlockSpec((planes, ROWS, depth, levels), lambda i, odd_ref: (0, i, 0, 0))

    def ends(planes):
        return pl.BlockSpec((planes, ROWS, levels), lambda i, odd_ref: (0, i, 0))

    half = rows // ROWS // 2
    half_ends = [
        pl.BlockSpec((4, ROWS, levels), lambda i, odd_ref: (0, jnp.minimum(i, half - 1), 0)),
        pl.BlockSpec((4, ROWS, levels), lambda i, odd_ref: (0, jnp.maximum(i - half, 0), 0)),
    ]
    face = pl.BlockSpec((ROWS, depth, levels), lambda i, odd_ref: (i, 0, 0))
    out_specs = [face, face, block(4 if last else 2)]
    out_shape = [struct(*o.shape), struct(*o.shape), struct(4 if last else 2, *o.shape)]
    if not last:
        out_specs += [fixed(2, depth, levels)] * 2 + [ends(2)] * 2
        out_shape += [struct(2, depth, levels)] * 2 + [struct(2, rows, levels)] * 2
    return pl.pallas_call(
        functools.partial(partial_kernel, first, last),
        grid_spec=pltpu.PrefetchScalarGridSpec(
            num_scalar_prefetch=1,
            grid=(rows // ROWS,),
            in_specs=specs(None)
            + specs(middle(1))
            + specs(middle(2))
            + specs(None)
            + [block(4), fixed(4, depth, levels), fixed(4, depth, levels), ends(4), *half_ends],
            out_specs=out_specs,
        ),
        out_shape=out_shape,
        compiler_params=pltpu.CompilerParams(vmem_limit_bytes=VMEM),
        cost_estimate=pl.CostEstimate(flops=60_000_000, bytes_accessed=40_000_000, transcendentals=0),
        name="partial_step",
    )(odd, *([o] * 3), *([mid] * 6), *([e] * 3), inverse, *halo_ends)


def z_ends_of(odd_ref, face):
    low, high = face[:, 0, :], face[:, face.shape[1] - 1, :]
    pz_odd = odd_ref[1] == 1
    return jnp.where(pz_odd, low, high), jnp.where(pz_odd, high, low)


def finish_even_kernel(odd_ref, part, halo, face, x_ends, z_ends):
    i, blocks = pl.program_id(0), pl.num_programs(0)
    face[...] = part[...] + 0.1 * halo[...]
    z_ends[0], z_ends[1] = z_ends_of(odd_ref, face)

    @pl.when(i == 0)
    def _():
        x_ends[0] = face[0]

    @pl.when(i == blocks - 1)
    def _():
        x_ends[1] = face[TILE - 1]


def finish_even(odd, part, halo):
    rows, depth, levels = part.shape
    face = pl.BlockSpec((TILE, depth, levels), lambda i, _: (i, 0, 0))
    return pl.pallas_call(
        finish_even_kernel,
        grid_spec=pltpu.PrefetchScalarGridSpec(
            num_scalar_prefetch=1,
            grid=(rows // TILE,),
            in_specs=[face, face],
            out_specs=[face, fixed(2, depth, levels), pl.BlockSpec((2, TILE, levels), lambda i, _: (0, i, 0))],
        ),
        out_shape=[struct(*part.shape), struct(2, depth, levels), struct(2, rows, levels)],
        compiler_params=pltpu.CompilerParams(vmem_limit_bytes=VMEM),
        cost_estimate=pl.CostEstimate(flops=6_000_000, bytes_accessed=9_500_000, transcendentals=0),
        name="finish_even",
    )(odd, part, halo)


def odd_halo(i, halo, relayed, store):
    straight = DIRECT // halo.shape[0]

    @pl.when(i < straight)
    def _():
        store(halo[...])

    @pl.when(i >= straight)
    def _():
        store(relayed[0][...] + relayed[1][...] + relayed[2][...])


def odd_halo_specs(depth, levels, tile):
    straight = DIRECT // tile
    top = pl.BlockSpec((tile, depth, levels), lambda i, *_: (jnp.minimum(i, straight - 1), 0, 0))
    rest = pl.BlockSpec((tile, depth, levels), lambda i, *_: (jnp.maximum(i - straight, 0), 0, 0))
    return top, rest


def finish_odd_kernel(odd_ref, part, halo, r0, r1, r2, mx_low, mx_high, mz_even, mz_odd, ex, ez, *outs):
    face, top, rest, x_low, x_high, z_even, z_odd = outs
    i, blocks = pl.program_id(0), pl.num_programs(0)

    def store(h):
        face[...] = part[...] + 0.1 * h

    odd_halo(i, halo, (r0, r1, r2), store)

    @pl.when(i < DIRECT // TILE)
    def _():
        top[...] = face[...]

    @pl.when(i >= DIRECT // TILE)
    def _():
        rest[...] = face[...]

    z_even[0], z_odd[0] = z_ends_of(odd_ref, face)
    for k, (z_out, z_mid) in enumerate(((z_even, mz_even), (z_odd, mz_odd))):
        z_out[1:3] = z_mid[...]
        z_out[3] = ez[k]

    @pl.when(i == 0)
    def _():
        x_low[0] = face[0]
        x_low[1:3] = mx_low[...]
        x_low[3] = ex[0]

    @pl.when(i == blocks - 1)
    def _():
        x_high[0] = face[TILE - 1]
        x_high[1:3] = mx_high[...]
        x_high[3] = ex[1]


def finish_odd(odd, part, halo, relayed, mids, ex, ez):
    rows, depth, levels = part.shape
    face = pl.BlockSpec((TILE, depth, levels), lambda i, _: (i, 0, 0))
    top, rest = odd_halo_specs(depth, levels, TILE)

    def ends(planes):
        return pl.BlockSpec((planes, TILE, levels), lambda i, _: (0, i, 0))

    x2, x4 = fixed(2, depth, levels), fixed(4, depth, levels)
    return pl.pallas_call(
        finish_odd_kernel,
        grid_spec=pltpu.PrefetchScalarGridSpec(
            num_scalar_prefetch=1,
            grid=(rows // TILE,),
            in_specs=[face, top, rest, rest, rest, x2, x2, ends(2), ends(2), x2, ends(2)],
            out_specs=[face, top, rest, x4, x4, ends(4), ends(4)],
        ),
        out_shape=[struct(*part.shape), struct(DIRECT, depth, levels), struct(rows - DIRECT, depth, levels)]
        + [struct(4, depth, levels)] * 2
        + [struct(4, rows, levels)] * 2,
        compiler_params=pltpu.CompilerParams(vmem_limit_bytes=VMEM),
        cost_estimate=pl.CostEstimate(flops=6_000_000, bytes_accessed=12_600_000, transcendentals=0),
        name="finish_odd",
    )(odd, part, halo, *relayed, *mids, ex, ez)


def place_even_kernel(at_ref, part, halo, whole, out):
    out[0] = part[...] + 0.1 * halo[...]


def place_odd_kernel(at_ref, part, halo, r0, r1, r2, whole, out):
    def store(h):
        out[0] = part[...] + 0.1 * h

    odd_halo(pl.program_id(0), halo, (r0, r1, r2), store)


def place(kernel, at, part, halos, whole, specs):
    rows, depth, levels = part.shape
    face = pl.BlockSpec((ROWS, depth, levels), lambda i, at_ref: (i, 0, 0))
    return pl.pallas_call(
        kernel,
        grid_spec=pltpu.PrefetchScalarGridSpec(
            num_scalar_prefetch=1,
            grid=(rows // ROWS,),
            in_specs=[face, *(specs or [face]), pl.BlockSpec(memory_space=pl.ANY)],
            out_specs=pl.BlockSpec((1, ROWS, depth, levels), lambda i, at_ref: (at_ref[0], i, 0, 0)),
        ),
        out_shape=struct(*whole.shape),
        input_output_aliases={2 + len(halos): 0},
        compiler_params=pltpu.CompilerParams(vmem_limit_bytes=VMEM),
        cost_estimate=pl.CostEstimate(flops=6_000_000, bytes_accessed=9_500_000, transcendentals=0),
        name="place",
    )(at.astype(jnp.int32).reshape(1), part, *halos, whole)


def pick_kernel(at_ref, density, *outs_and_sems):
    outs, sems = outs_and_sems[:-1], outs_and_sems[-1]
    plane = density.at[at_ref[0]]
    starts = [0, 0, DIRECT]
    copies = [
        pltpu.make_async_copy(plane.at[pl.ds(starts[k], out.shape[0])], out, sems.at[k]) for k, out in enumerate(outs)
    ]
    for copy in copies:
        copy.start()
    for copy in copies:
        copy.wait()


def pick(density, at, parts, grant):
    _, rows, depth, levels = density.shape
    sizes = (rows, DIRECT, rows - DIRECT)[:parts]
    return pl.pallas_call(
        pick_kernel,
        in_specs=[pl.BlockSpec(memory_space=pltpu.SMEM), pl.BlockSpec(memory_space=pltpu.HBM)],
        out_specs=[pl.BlockSpec(memory_space=pltpu.VMEM)] * parts,
        out_shape=[struct(size, depth, levels) for size in sizes],
        scratch_shapes=[pltpu.SemaphoreType.DMA((parts,))],
        compiler_params=pltpu.CompilerParams(vmem_limit_bytes=grant * 1024 * 1024),
        cost_estimate=pl.CostEstimate(flops=1_000_000, bytes_accessed=6_300_000, transcendentals=0),
    )(at.astype(jnp.int32).reshape(1), density)


def local(density, inverse):
    odd, pz_odd = lax.axis_index("py") % 2, lax.axis_index("pz") % 2
    odd_ref = jnp.stack([odd, pz_odd]).astype(jnp.int32)
    e_plane, o_plane = 3 * (1 - odd), 3 * odd
    (e,) = pick(density, e_plane, 1, 50)
    e_halo = lax.ppermute(e, "py", EVEN_CUTS)
    o, top, rest = pick(density, o_plane, 3, 46)
    mid = density
    rows, depth, levels = o.shape
    x_low, x_high = density[:, 0], density[:, rows - 1]
    z_low, z_high = density[:, :, 0], density[:, :, depth - 1]
    z_even, z_odd = jnp.where(pz_odd == 1, z_low, z_high), jnp.where(pz_odd == 1, z_high, z_low)
    up = [(k, k + 1) for k in range(3)]
    down = [(b, a) for a, b in up]
    half = rows // 2
    for step in range(STEPS):
        z_by = lax.ppermute(z_odd[:, half:], "pz", [(1, 3), (2, 0)])
        z_even = lax.ppermute(z_even, "pz", [(0, 1), (1, 0), (2, 3), (3, 2)])
        z_odd = lax.ppermute(z_odd[:, :half], "pz", [(1, 2), (2, 1)])
        z_by = lax.ppermute(z_by, "pz", [(3, 2), (0, 1)])
        relayed = []
        for to, _ in RELAYS:
            relayed.append(lax.ppermute(rest, "py", to))
        px = [lax.ppermute(x_high, "px", up), lax.ppermute(x_low, "px", down)]
        o_halo = lax.ppermute(top, "py", ODD_CUTS)
        for k, (_, on) in enumerate(RELAYS):
            relayed[k] = lax.ppermute(relayed[k], "py", on)
        ends = [*px, z_even, z_odd, z_by]
        o_part, e_part, mid, *mids = partial_step(step, odd_ref, o, mid, e, inverse, ends)
        if step == STEPS - 1:
            break
        e, ex, ez = finish_even(odd_ref, e_part, e_halo)
        e_halo = lax.ppermute(e, "py", EVEN_CUTS)
        o, top, rest, x_low, x_high, z_even, z_odd = finish_odd(odd_ref, o_part, o_halo, relayed, mids, ex, ez)
    out = place(place_even_kernel, e_plane, e_part, (e_halo,), mid, None)
    halo, relay = odd_halo_specs(depth, levels, ROWS)
    return place(place_odd_kernel, o_plane, o_part, (o_halo, *relayed), out, [halo] + [relay] * 3)


def solution(mesh):
    spec = P("py", "px", "pz", None)
    return jax.shard_map(local, mesh=mesh, in_specs=(spec, spec), out_specs=spec, check_vma=False)
```

```python
import functools

import jax
import jax.numpy as jnp
from jax import lax
from jax.experimental import pallas as pl
from jax.experimental.pallas import tpu as pltpu
from jax.sharding import PartitionSpec as P


STEPS = 3
ROWS = 8
TILE = 16
DIRECT = 48

EVEN_CUTS = [(0, 1), (1, 0), (2, 3), (3, 2), (4, 5), (5, 4), (6, 7), (7, 6)]
ODD_CUTS = [(1, 2), (2, 1), (3, 4), (4, 3), (5, 6), (6, 5)]
RELAYS = [
    ([(2, 0), (5, 7)], [(0, 1), (7, 6)]),
    ([(4, 0), (3, 7)], [(0, 3), (7, 4)]),
    ([(6, 0), (1, 7)], [(0, 5), (7, 2)]),
]
VMEM = 20 * 1024 * 1024


def struct(*shape):
    return jax.ShapeDtypeStruct(shape, jnp.float32)


def fixed(*shape):
    return pl.BlockSpec(shape, lambda i, *_: (0,) * len(shape))


def partial_kernel(first, last, odd_ref, *refs):
    planes = [refs[3 * s : 3 * s + 3] for s in range(4)]
    inverse, px_low, px_high, z_even, z_odd, z_on = refs[12:18]
    part_o, part_e, kept, mx_low, mx_high, mz_even, mz_odd = (refs[18:] + (None,) * 4)[:7]
    i, blocks = pl.program_id(0), pl.num_programs(0)
    odd, pz_odd = odd_ref[0], odd_ref[1] == 1
    shape = px_low.shape[1:]
    depth = shape[0]
    z = lax.broadcasted_iota(jnp.int32, shape, 0)

    def stored(s):
        return jnp.where(odd == 1, 3 - s, s)

    def edge(s):
        return stored(s) if first else s

    def main(s, r):
        ref = planes[s][0]
        return ref[r] if len(ref.shape) == 3 else ref[0, r]

    def one_row(r, before, after):
        for s in range(4):
            c = main(s, r)
            over_even, over_odd, over_on = (v[edge(s), pl.ds(r, 1), :] for v in (z_even, z_odd, z_on))
            over_odd = jnp.where(2 * i < blocks, over_odd, over_on)
            below = jnp.where(z == 0, jnp.where(pz_odd, over_even, over_odd), pltpu.roll(c, 1, 0))
            above = jnp.where(z == depth - 1, jnp.where(pz_odd, over_odd, over_even), pltpu.roll(c, depth - 1, 0))
            total = (before(s) + after(s)) + (below + above)
            if s > 0:
                total = total + main(s - 1, r)
            if s < 3:
                total = total + main(s + 1, r)
            value = c * (0.6 - 0.2 * c * inverse[stored(s), r]) + 0.1 * total
            if s == 0:
                part_o[r] = value
            elif s == 3:
                part_e[r] = value
            elif last:
                kept[stored(s), r] = value
            else:
                kept[s - 1, r] = value
                low, high = value[0:1, :], value[depth - 1 : depth, :]
                mz_even[s - 1, pl.ds(r, 1), :] = jnp.where(pz_odd, low, high)
                mz_odd[s - 1, pl.ds(r, 1), :] = jnp.where(pz_odd, high, low)

    def earlier(s):
        return jnp.where(i == 0, px_low[edge(s)], planes[s][1][...].reshape(shape))

    def later(s):
        return jnp.where(i == blocks - 1, px_high[edge(s)], planes[s][2][...].reshape(shape))

    one_row(0, earlier, lambda s: main(s, 1))

    @pl.loop(1, ROWS - 1)
    def _(r):
        one_row(r, lambda s: main(s, r - 1), lambda s: main(s, r + 1))

    one_row(ROWS - 1, lambda s: main(s, ROWS - 2), later)
    if not last:

        @pl.when(i == 0)
        def _():
            mx_low[...] = kept[:, 0]

        @pl.when(i == blocks - 1)
        def _():
            mx_high[...] = kept[:, ROWS - 1]


def partial_step(step, odd, o, mid, e, inverse, halo_ends):
    first, last = step == 0, step == STEPS - 1
    rows, depth, levels = o.shape

    def specs(plane):
        if plane is None:
            shape, at = (lambda k: (k, depth, levels)), (lambda j, odd_ref: (j, 0, 0))
        else:
            shape, at = (lambda k: (1, k, depth, levels)), (lambda j, odd_ref: (plane(odd_ref), j, 0, 0))
        return [
            pl.BlockSpec(shape(ROWS), lambda i, odd_ref: at(i, odd_ref)),
            pl.BlockSpec(shape(1), lambda i, odd_ref: at(jnp.maximum(i * ROWS - 1, 0), odd_ref)),
            pl.BlockSpec(shape(1), lambda i, odd_ref: at(jnp.minimum(i * ROWS + ROWS, rows - 1), odd_ref)),
        ]

    def middle(s):
        if first:
            return lambda odd_ref: jnp.where(odd_ref[0] == 1, 3 - s, s)
        return lambda odd_ref: s - 1

    def block(planes):
        return pl.BlockSpec((planes, ROWS, depth, levels), lambda i, odd_ref: (0, i, 0, 0))

    def ends(planes):
        return pl.BlockSpec((planes, ROWS, levels), lambda i, odd_ref: (0, i, 0))

    half = rows // ROWS // 2
    half_ends = [
        pl.BlockSpec((4, ROWS, levels), lambda i, odd_ref: (0, jnp.minimum(i, half - 1), 0)),
        pl.BlockSpec((4, ROWS, levels), lambda i, odd_ref: (0, jnp.maximum(i - half, 0), 0)),
    ]
    face = pl.BlockSpec((ROWS, depth, levels), lambda i, odd_ref: (i, 0, 0))
    out_specs = [face, face, block(4 if last else 2)]
    out_shape = [struct(*o.shape), struct(*o.shape), struct(4 if last else 2, *o.shape)]
    if not last:
        out_specs += [fixed(2, depth, levels)] * 2 + [ends(2)] * 2
        out_shape += [struct(2, depth, levels)] * 2 + [struct(2, rows, levels)] * 2
    return pl.pallas_call(
        functools.partial(partial_kernel, first, last),
        grid_spec=pltpu.PrefetchScalarGridSpec(
            num_scalar_prefetch=1,
            grid=(rows // ROWS,),
            in_specs=specs(None)
            + specs(middle(1))
            + specs(middle(2))
            + specs(None)
            + [block(4), fixed(4, depth, levels), fixed(4, depth, levels), ends(4), *half_ends],
            out_specs=out_specs,
        ),
        out_shape=out_shape,
        compiler_params=pltpu.CompilerParams(vmem_limit_bytes=VMEM),
        cost_estimate=pl.CostEstimate(flops=60_000_000, bytes_accessed=40_000_000, transcendentals=0),
        name="partial_step",
    )(odd, *([o] * 3), *([mid] * 6), *([e] * 3), inverse, *halo_ends)


def z_ends_of(odd_ref, face):
    low, high = face[:, 0, :], face[:, face.shape[1] - 1, :]
    pz_odd = odd_ref[1] == 1
    return jnp.where(pz_odd, low, high), jnp.where(pz_odd, high, low)


def finish_even_kernel(odd_ref, part, halo, face, x_ends, z_ends):
    i, blocks = pl.program_id(0), pl.num_programs(0)
    face[...] = part[...] + 0.1 * halo[...]
    z_ends[0], z_ends[1] = z_ends_of(odd_ref, face)

    @pl.when(i == 0)
    def _():
        x_ends[0] = face[0]

    @pl.when(i == blocks - 1)
    def _():
        x_ends[1] = face[TILE - 1]


def finish_even(odd, part, halo):
    rows, depth, levels = part.shape
    face = pl.BlockSpec((TILE, depth, levels), lambda i, _: (i, 0, 0))
    return pl.pallas_call(
        finish_even_kernel,
        grid_spec=pltpu.PrefetchScalarGridSpec(
            num_scalar_prefetch=1,
            grid=(rows // TILE,),
            in_specs=[face, face],
            out_specs=[face, fixed(2, depth, levels), pl.BlockSpec((2, TILE, levels), lambda i, _: (0, i, 0))],
        ),
        out_shape=[struct(*part.shape), struct(2, depth, levels), struct(2, rows, levels)],
        compiler_params=pltpu.CompilerParams(vmem_limit_bytes=VMEM),
        cost_estimate=pl.CostEstimate(flops=6_000_000, bytes_accessed=9_500_000, transcendentals=0),
        name="finish_even",
    )(odd, part, halo)


def odd_halo(i, halo, relayed, store):
    straight = DIRECT // TILE

    @pl.when(i < straight)
    def _():
        store(halo[...])

    @pl.when(i >= straight)
    def _():
        store(relayed[0][...] + relayed[1][...] + relayed[2][...])


def odd_halo_specs(depth, levels):
    straight = DIRECT // TILE
    top = pl.BlockSpec((TILE, depth, levels), lambda i, *_: (jnp.minimum(i, straight - 1), 0, 0))
    rest = pl.BlockSpec((TILE, depth, levels), lambda i, *_: (jnp.maximum(i - straight, 0), 0, 0))
    return top, rest


def finish_odd_kernel(odd_ref, part, halo, r0, r1, r2, mx_low, mx_high, mz_even, mz_odd, ex, ez, *outs):
    face, top, rest, x_low, x_high, z_even, z_odd = outs
    i, blocks = pl.program_id(0), pl.num_programs(0)

    def store(h):
        face[...] = part[...] + 0.1 * h

    odd_halo(i, halo, (r0, r1, r2), store)

    @pl.when(i < DIRECT // TILE)
    def _():
        top[...] = face[...]

    @pl.when(i >= DIRECT // TILE)
    def _():
        rest[...] = face[...]

    z_even[0], z_odd[0] = z_ends_of(odd_ref, face)
    for k, (z_out, z_mid) in enumerate(((z_even, mz_even), (z_odd, mz_odd))):
        z_out[1:3] = z_mid[...]
        z_out[3] = ez[k]

    @pl.when(i == 0)
    def _():
        x_low[0] = face[0]
        x_low[1:3] = mx_low[...]
        x_low[3] = ex[0]

    @pl.when(i == blocks - 1)
    def _():
        x_high[0] = face[TILE - 1]
        x_high[1:3] = mx_high[...]
        x_high[3] = ex[1]


def finish_odd(odd, part, halo, relayed, mids, ex, ez):
    rows, depth, levels = part.shape
    face = pl.BlockSpec((TILE, depth, levels), lambda i, _: (i, 0, 0))
    top, rest = odd_halo_specs(depth, levels)

    def ends(planes):
        return pl.BlockSpec((planes, TILE, levels), lambda i, _: (0, i, 0))

    x2, x4 = fixed(2, depth, levels), fixed(4, depth, levels)
    return pl.pallas_call(
        finish_odd_kernel,
        grid_spec=pltpu.PrefetchScalarGridSpec(
            num_scalar_prefetch=1,
            grid=(rows // TILE,),
            in_specs=[face, top, rest, rest, rest, x2, x2, ends(2), ends(2), x2, ends(2)],
            out_specs=[face, top, rest, x4, x4, ends(4), ends(4)],
        ),
        out_shape=[struct(*part.shape), struct(DIRECT, depth, levels), struct(rows - DIRECT, depth, levels)]
        + [struct(4, depth, levels)] * 2
        + [struct(4, rows, levels)] * 2,
        compiler_params=pltpu.CompilerParams(vmem_limit_bytes=VMEM),
        cost_estimate=pl.CostEstimate(flops=6_000_000, bytes_accessed=12_600_000, transcendentals=0),
        name="finish_odd",
    )(odd, part, halo, *relayed, *mids, ex, ez)


def place_kernel(at_ref, part, *refs):
    halos, (_, out, done, sems) = refs[:-4], refs[-4:]
    plane = out.at[at_ref[0]]
    copies = []
    for k in range(part.shape[0] // TILE):
        own = pl.ds(k * TILE, TILE)
        if len(halos) == 1:
            halo = halos[0][own]
        elif k < DIRECT // TILE:
            halo = halos[0][own]
        else:
            rest = pl.ds(k * TILE - DIRECT, TILE)
            halo = halos[1][rest] + halos[2][rest] + halos[3][rest]
        done[own] = part[own] + 0.1 * halo
        copies.append(pltpu.make_async_copy(done.at[own], plane.at[own], sems.at[k]))
        copies[-1].start()
    for copy in copies:
        copy.wait()


def place(at, part, halos, whole):
    held = pl.BlockSpec(memory_space=pltpu.VMEM)
    return pl.pallas_call(
        place_kernel,
        in_specs=[pl.BlockSpec(memory_space=pltpu.SMEM), held]
        + [held] * len(halos)
        + [pl.BlockSpec(memory_space=pltpu.HBM)],
        out_specs=pl.BlockSpec(memory_space=pltpu.HBM),
        out_shape=struct(*whole.shape),
        scratch_shapes=[pltpu.VMEM(part.shape, jnp.float32), pltpu.SemaphoreType.DMA((part.shape[0] // TILE,))],
        input_output_aliases={2 + len(halos): 0},
        compiler_params=pltpu.CompilerParams(vmem_limit_bytes=VMEM),
        cost_estimate=pl.CostEstimate(flops=6_000_000, bytes_accessed=9_500_000, transcendentals=0),
        name="place",
    )(at.astype(jnp.int32).reshape(1), part, *halos, whole)


def pick_kernel(starts, at_ref, density, *outs_and_sems):
    outs, sems = outs_and_sems[:-1], outs_and_sems[-1]
    plane = density.at[at_ref[0]]
    copies = [
        pltpu.make_async_copy(plane.at[pl.ds(starts[k], out.shape[0])], out, sems.at[k]) for k, out in enumerate(outs)
    ]
    for copy in copies:
        copy.start()
    for copy in copies:
        copy.wait()


def pick(density, at, spans, grant):
    _, _, depth, levels = density.shape
    return pl.pallas_call(
        functools.partial(pick_kernel, [start for start, _ in spans]),
        in_specs=[pl.BlockSpec(memory_space=pltpu.SMEM), pl.BlockSpec(memory_space=pltpu.HBM)],
        out_specs=[pl.BlockSpec(memory_space=pltpu.VMEM)] * len(spans),
        out_shape=[struct(stop - start, depth, levels) for start, stop in spans],
        scratch_shapes=[pltpu.SemaphoreType.DMA((len(spans),))],
        compiler_params=pltpu.CompilerParams(vmem_limit_bytes=grant * 1024 * 1024),
        cost_estimate=pl.CostEstimate(flops=1_000_000, bytes_accessed=6_300_000, transcendentals=0),
    )(at.astype(jnp.int32).reshape(1), density)


def local(density, inverse):
    odd, pz_odd = lax.axis_index("py") % 2, lax.axis_index("pz") % 2
    odd_ref = jnp.stack([odd, pz_odd]).astype(jnp.int32)
    e_plane, o_plane = 3 * (1 - odd), 3 * odd
    rows = density.shape[1]
    (e_first,) = pick(density, e_plane, [(0, TILE)], 52)
    first_halo = lax.ppermute(e_first, "py", EVEN_CUTS)
    e, e_rest = pick(density, e_plane, [(0, rows), (TILE, rows)], 50)
    e_halo = lax.ppermute(e_rest, "py", EVEN_CUTS)
    o, top, rest = pick(density, o_plane, [(0, rows), (0, DIRECT), (DIRECT, rows)], 46)
    mid = density
    rows, depth, _ = o.shape
    x_low, x_high = density[:, 0], density[:, rows - 1]
    z_low, z_high = density[:, :, 0], density[:, :, depth - 1]
    z_even, z_odd = jnp.where(pz_odd == 1, z_low, z_high), jnp.where(pz_odd == 1, z_high, z_low)
    up = [(k, k + 1) for k in range(3)]
    down = [(b, a) for a, b in up]
    half = rows // 2
    for step in range(STEPS):
        z_by = lax.ppermute(z_odd[:, half:], "pz", [(1, 3), (2, 0)])
        z_even = lax.ppermute(z_even, "pz", [(0, 1), (1, 0), (2, 3), (3, 2)])
        z_odd = lax.ppermute(z_odd[:, :half], "pz", [(1, 2), (2, 1)])
        z_by = lax.ppermute(z_by, "pz", [(3, 2), (0, 1)])
        relayed = []
        for to, _ in RELAYS:
            relayed.append(lax.ppermute(rest, "py", to))
        px = [lax.ppermute(x_high, "px", up), lax.ppermute(x_low, "px", down)]
        o_halo = lax.ppermute(top, "py", ODD_CUTS)
        for k, (_, on) in enumerate(RELAYS):
            relayed[k] = lax.ppermute(relayed[k], "py", on)
        ends = [*px, z_even, z_odd, z_by]
        o_part, e_part, mid, *mids = partial_step(step, odd_ref, o, mid, e, inverse, ends)
        if step == STEPS - 1:
            break
        if step == 0:
            e_halo = jnp.concatenate([first_halo, e_halo])
        e, ex, ez = finish_even(odd_ref, e_part, e_halo)
        e_halo = lax.ppermute(e, "py", EVEN_CUTS)
        o, top, rest, x_low, x_high, z_even, z_odd = finish_odd(odd_ref, o_part, o_halo, relayed, mids, ex, ez)
    out = place(e_plane, e_part, (e_halo,), mid)
    return place(o_plane, o_part, (o_halo, *relayed), out)


def solution(mesh):
    spec = P("py", "px", "pz", None)
    return jax.shard_map(local, mesh=mesh, in_specs=(spec, spec), out_specs=spec, check_vma=False)
```

```python
import functools

import jax
import jax.numpy as jnp
from jax import lax
from jax.experimental import pallas as pl
from jax.experimental.pallas import tpu as pltpu
from jax.sharding import PartitionSpec as P


STEPS = 3
ROWS = 8
TILE = 16
EARLY = 16
DIRECT = 48

EVEN_CUTS = [(0, 1), (1, 0), (2, 3), (3, 2), (4, 5), (5, 4), (6, 7), (7, 6)]
ODD_CUTS = [(1, 2), (2, 1), (3, 4), (4, 3), (5, 6), (6, 5)]
RELAYS = [
    ([(6, 0), (1, 7)], [(0, 5), (7, 2)]),
    ([(4, 0), (3, 7)], [(0, 3), (7, 4)]),
    ([(2, 0), (5, 7)], [(0, 1), (7, 6)]),
]
CORNERS_UP = [(4 * a + k, 4 * b + k + 1) for a, b in EVEN_CUTS for k in range(3)]
CORNERS_DOWN = [(4 * a + k + 1, 4 * b + k) for a, b in EVEN_CUTS for k in range(3)]
VMEM = 20 * 1024 * 1024
PART_VMEM = 24 * 1024 * 1024


def struct(*shape):
    return jax.ShapeDtypeStruct(shape, jnp.float32)


def fixed(*shape):
    return pl.BlockSpec(shape, lambda i, *_: (0,) * len(shape))


def partial_kernel(first, last, odd_ref, *refs):
    planes = [refs[3 * s : 3 * s + 3] for s in range(4)]
    inverse, px_low, px_high, z_even, z_odd, z_on = refs[12:18]
    part_o, part_e, kept, mx_low, mx_high, mz_even, mz_odd = (refs[18:] + (None,) * 4)[:7]
    i, blocks = pl.program_id(0), pl.num_programs(0)
    odd, pz_odd = odd_ref[0], odd_ref[1] == 1
    shape = px_low.shape[1:]
    depth = shape[0]
    z = lax.broadcasted_iota(jnp.int32, shape, 0)

    def stored(s):
        return jnp.where(odd == 1, 3 - s, s)

    def edge(s):
        return stored(s) if first else s

    def z_edge(s):
        return stored(s) - odd if first else s

    def main(s, r):
        ref = planes[s][0]
        return ref[r] if len(ref.shape) == 3 else ref[0, r]

    def one_row(r, before, after):
        for s in range(4):
            c = main(s, r)
            if s < 3:
                over_even, over_odd, over_on = (v[z_edge(s), pl.ds(r, 1), :] for v in (z_even, z_odd, z_on))
                over_odd = jnp.where(2 * i < blocks, over_odd, over_on)
                low, high = jnp.where(pz_odd, over_even, over_odd), jnp.where(pz_odd, over_odd, over_even)
            else:
                low = high = 0.0
            below = jnp.where(z == 0, low, pltpu.roll(c, 1, 0))
            above = jnp.where(z == depth - 1, high, pltpu.roll(c, depth - 1, 0))
            total = (before(s) + after(s)) + (below + above)
            if s > 0:
                total = total + main(s - 1, r)
            if s < 3:
                total = total + main(s + 1, r)
            value = c * (0.6 - 0.2 * c * inverse[stored(s), r]) + 0.1 * total
            if s == 0:
                part_o[r] = value
            elif s == 3:
                part_e[r] = value
            elif last:
                kept[stored(s), r] = value
            else:
                kept[s - 1, r] = value
                low, high = value[0:1, :], value[depth - 1 : depth, :]
                mz_even[s - 1, pl.ds(r, 1), :] = jnp.where(pz_odd, low, high)
                mz_odd[s - 1, pl.ds(r, 1), :] = jnp.where(pz_odd, high, low)

    def earlier(s):
        return jnp.where(i == 0, px_low[edge(s)], planes[s][1][...].reshape(shape))

    def later(s):
        return jnp.where(i == blocks - 1, px_high[edge(s)], planes[s][2][...].reshape(shape))

    one_row(0, earlier, lambda s: main(s, 1))

    @pl.loop(1, ROWS - 1)
    def _(r):
        one_row(r, lambda s: main(s, r - 1), lambda s: main(s, r + 1))

    one_row(ROWS - 1, lambda s: main(s, ROWS - 2), later)
    if not last:

        @pl.when(i == 0)
        def _():
            mx_low[...] = kept[:, 0]

        @pl.when(i == blocks - 1)
        def _():
            mx_high[...] = kept[:, ROWS - 1]


def partial_step(step, odd, o, mid, e, inverse, halo_ends):
    first, last = step == 0, step == STEPS - 1
    rows, depth, levels = o.shape

    def specs(plane):
        if plane is None:
            shape, at = (lambda k: (k, depth, levels)), (lambda j, odd_ref: (j, 0, 0))
        else:
            shape, at = (lambda k: (1, k, depth, levels)), (lambda j, odd_ref: (plane(odd_ref), j, 0, 0))
        return [
            pl.BlockSpec(shape(ROWS), lambda i, odd_ref: at(i, odd_ref)),
            pl.BlockSpec(shape(1), lambda i, odd_ref: at(jnp.maximum(i * ROWS - 1, 0), odd_ref)),
            pl.BlockSpec(shape(1), lambda i, odd_ref: at(jnp.minimum(i * ROWS + ROWS, rows - 1), odd_ref)),
        ]

    def middle(s):
        if first:
            return lambda odd_ref: jnp.where(odd_ref[0] == 1, 3 - s, s)
        return lambda odd_ref: s - 1

    def block(planes):
        return pl.BlockSpec((planes, ROWS, depth, levels), lambda i, odd_ref: (0, i, 0, 0))

    def ends(planes):
        return pl.BlockSpec((planes, ROWS, levels), lambda i, odd_ref: (0, i, 0))

    half = rows // ROWS // 2
    half_ends = [
        pl.BlockSpec((3, ROWS, levels), lambda i, odd_ref: (0, jnp.minimum(i, half - 1), 0)),
        pl.BlockSpec((3, ROWS, levels), lambda i, odd_ref: (0, jnp.maximum(i - half, 0), 0)),
    ]
    face = pl.BlockSpec((ROWS, depth, levels), lambda i, odd_ref: (i, 0, 0))
    out_specs = [face, face, block(4 if last else 2)]
    out_shape = [struct(*o.shape), struct(*o.shape), struct(4 if last else 2, *o.shape)]
    if not last:
        out_specs += [fixed(2, depth, levels)] * 2 + [ends(2)] * 2
        out_shape += [struct(2, depth, levels)] * 2 + [struct(2, rows, levels)] * 2
    return pl.pallas_call(
        functools.partial(partial_kernel, first, last),
        grid_spec=pltpu.PrefetchScalarGridSpec(
            num_scalar_prefetch=1,
            grid=(rows // ROWS,),
            in_specs=specs(None)
            + specs(middle(1))
            + specs(middle(2))
            + specs(None)
            + [block(4), fixed(4, depth, levels), fixed(4, depth, levels), ends(3), *half_ends],
            out_specs=out_specs,
        ),
        out_shape=out_shape,
        compiler_params=pltpu.CompilerParams(vmem_limit_bytes=PART_VMEM),
        cost_estimate=pl.CostEstimate(flops=60_000_000, bytes_accessed=40_000_000, transcendentals=0),
        name="partial_step",
    )(odd, *([o] * 3), *([mid] * 6), *([e] * 3), inverse, *halo_ends)


def z_ends_of(odd_ref, face):
    low, high = face[:, 0, :], face[:, face.shape[1] - 1, :]
    pz_odd = odd_ref[1] == 1
    return jnp.where(pz_odd, low, high), jnp.where(pz_odd, high, low)


def finish_even_kernel(part, halo, low, high, face, x_ends):
    i, blocks = pl.program_id(0), pl.num_programs(0)
    depth = face.shape[1]
    face[...] = part[...] + 0.1 * halo[...]
    face[:, 0, :] = face[:, 0, :] + 0.1 * low[...]
    face[:, depth - 1, :] = face[:, depth - 1, :] + 0.1 * high[...]

    @pl.when(i == 0)
    def _():
        x_ends[0] = face[0]

    @pl.when(i == blocks - 1)
    def _():
        x_ends[1] = face[TILE - 1]


def finish_even(part, halo, low, high):
    rows, depth, levels = part.shape
    face = pl.BlockSpec((TILE, depth, levels), lambda i: (i, 0, 0))
    column = pl.BlockSpec((TILE, levels), lambda i: (i, 0))
    return pl.pallas_call(
        finish_even_kernel,
        grid=(rows // TILE,),
        in_specs=[face, face, column, column],
        out_specs=[face, fixed(2, depth, levels)],
        out_shape=[struct(*part.shape), struct(2, depth, levels)],
        compiler_params=pltpu.CompilerParams(vmem_limit_bytes=VMEM),
        cost_estimate=pl.CostEstimate(flops=6_000_000, bytes_accessed=9_500_000, transcendentals=0),
        name="finish_even",
    )(part, halo, low, high)


def columns_kernel(halo, low, high):
    low[...] = halo[:, 0, :]
    high[...] = halo[:, halo.shape[1] - 1, :]


def columns(halo):
    rows, _, levels = halo.shape
    return pl.pallas_call(
        columns_kernel,
        in_specs=[pl.BlockSpec(memory_space=pltpu.VMEM)],
        out_specs=[pl.BlockSpec(memory_space=pltpu.VMEM)] * 2,
        out_shape=[struct(rows, levels)] * 2,
        compiler_params=pltpu.CompilerParams(vmem_limit_bytes=VMEM),
        cost_estimate=pl.CostEstimate(flops=1_000_000, bytes_accessed=100_000, transcendentals=0),
        name="columns",
    )(halo)


def odd_pieces():
    return ((0, EARLY // TILE), (EARLY // TILE, DIRECT // TILE), (DIRECT // TILE, None))


def in_piece(i, piece):
    return i >= piece[0] if piece[1] is None else (i >= piece[0]) & (i < piece[1])


def odd_specs(rows, depth, levels):
    def spec(start, stop):
        last = (rows // TILE if stop is None else stop) - start - 1
        return pl.BlockSpec((TILE, depth, levels), lambda i, *_: (jnp.clip(i - start, 0, last), 0, 0))

    return [spec(*piece) for piece in odd_pieces()]


def finish_odd_kernel(odd_ref, part, early, late, r0, r1, r2, mx_low, mx_high, mz_even, mz_odd, ex, *outs):
    face, *pieces, x_low, x_high, z_even, z_odd = outs
    i, blocks = pl.program_id(0), pl.num_programs(0)

    for (piece, out), halos in zip(zip(odd_pieces(), pieces), ((early,), (late,), (r0, r1, r2))):

        @pl.when(in_piece(i, piece))
        def _(out=out, halos=halos):
            face[...] = part[...] + 0.1 * sum((h[...] for h in halos[1:]), halos[0][...])
            out[...] = face[...]

    z_even[0], z_odd[0] = z_ends_of(odd_ref, face)
    z_even[1:3], z_odd[1:3] = mz_even[...], mz_odd[...]

    @pl.when(i == 0)
    def _():
        x_low[0] = face[0]
        x_low[1:3] = mx_low[...]
        x_low[3] = ex[0]

    @pl.when(i == blocks - 1)
    def _():
        x_high[0] = face[TILE - 1]
        x_high[1:3] = mx_high[...]
        x_high[3] = ex[1]


def finish_odd(odd, part, halos, relayed, mids, ex):
    rows, depth, levels = part.shape
    face = pl.BlockSpec((TILE, depth, levels), lambda i, _: (i, 0, 0))
    early, late, relay = odd_specs(rows, depth, levels)

    def ends(planes):
        return pl.BlockSpec((planes, TILE, levels), lambda i, _: (0, i, 0))

    x2, x4 = fixed(2, depth, levels), fixed(4, depth, levels)
    return pl.pallas_call(
        finish_odd_kernel,
        grid_spec=pltpu.PrefetchScalarGridSpec(
            num_scalar_prefetch=1,
            grid=(rows // TILE,),
            in_specs=[face, early, late, relay, relay, relay, x2, x2, ends(2), ends(2), x2],
            out_specs=[face, early, late, relay, x4, x4, ends(3), ends(3)],
        ),
        out_shape=[struct(*part.shape)]
        + [struct(size, depth, levels) for size in (EARLY, DIRECT - EARLY, rows - DIRECT)]
        + [struct(4, depth, levels)] * 2
        + [struct(3, rows, levels)] * 2,
        compiler_params=pltpu.CompilerParams(vmem_limit_bytes=VMEM),
        cost_estimate=pl.CostEstimate(flops=6_000_000, bytes_accessed=12_600_000, transcendentals=0),
        name="finish_odd",
    )(odd, part, *halos, *relayed, *mids, ex)


def place_kernel(at_ref, part, *refs):
    halos, (_, out, done, sems) = refs[:-4], refs[-4:]
    plane = out.at[at_ref[0]]
    copies = []
    for k in range(part.shape[0] // TILE):
        own = pl.ds(k * TILE, TILE)
        if len(halos) == 3:
            halo = halos[0][own]
        elif k * TILE < EARLY:
            halo = halos[0][own]
        elif k * TILE < DIRECT:
            halo = halos[1][pl.ds(k * TILE - EARLY, TILE)]
        else:
            rest = pl.ds(k * TILE - DIRECT, TILE)
            halo = halos[2][rest] + halos[3][rest] + halos[4][rest]
        done[own] = part[own] + 0.1 * halo
        if len(halos) == 3:
            for column, at in zip(halos[1:], (0, part.shape[1] - 1)):
                done[own, at, :] = done[own, at, :] + 0.1 * column[own]
        copies.append(pltpu.make_async_copy(done.at[own], plane.at[own], sems.at[k]))
        copies[-1].start()
    for copy in copies:
        copy.wait()


def place(at, part, halos, whole):
    held = pl.BlockSpec(memory_space=pltpu.VMEM)
    return pl.pallas_call(
        place_kernel,
        in_specs=[pl.BlockSpec(memory_space=pltpu.SMEM), held]
        + [held] * len(halos)
        + [pl.BlockSpec(memory_space=pltpu.HBM)],
        out_specs=pl.BlockSpec(memory_space=pltpu.HBM),
        out_shape=struct(*whole.shape),
        scratch_shapes=[pltpu.VMEM(part.shape, jnp.float32), pltpu.SemaphoreType.DMA((part.shape[0] // TILE,))],
        input_output_aliases={2 + len(halos): 0},
        compiler_params=pltpu.CompilerParams(vmem_limit_bytes=VMEM),
        cost_estimate=pl.CostEstimate(flops=6_000_000, bytes_accessed=9_500_000, transcendentals=0),
        name="place",
    )(at.astype(jnp.int32).reshape(1), part, *halos, whole)


def pick_kernel(starts, at_ref, density, *outs_and_sems):
    outs, sems = outs_and_sems[:-1], outs_and_sems[-1]
    plane = density.at[at_ref[0]]
    copies = [
        pltpu.make_async_copy(plane.at[pl.ds(starts[k], out.shape[0])], out, sems.at[k]) for k, out in enumerate(outs)
    ]
    for copy in copies:
        copy.start()
    for copy in copies:
        copy.wait()


def pick(density, at, spans, grant):
    _, _, depth, levels = density.shape
    return pl.pallas_call(
        functools.partial(pick_kernel, [start for start, _ in spans]),
        in_specs=[pl.BlockSpec(memory_space=pltpu.SMEM), pl.BlockSpec(memory_space=pltpu.HBM)],
        out_specs=[pl.BlockSpec(memory_space=pltpu.VMEM)] * len(spans),
        out_shape=[struct(stop - start, depth, levels) for start, stop in spans],
        scratch_shapes=[pltpu.SemaphoreType.DMA((len(spans),))],
        compiler_params=pltpu.CompilerParams(vmem_limit_bytes=grant * 1024 * 1024),
        cost_estimate=pl.CostEstimate(flops=1_000_000, bytes_accessed=6_300_000, transcendentals=0),
    )(at.astype(jnp.int32).reshape(1), density)


def local(density, inverse):
    odd, pz_odd = lax.axis_index("py") % 2, lax.axis_index("pz") % 2
    odd_ref = jnp.stack([odd, pz_odd]).astype(jnp.int32)
    e_plane, o_plane = 3 * (1 - odd), 3 * odd
    rows = density.shape[1]
    (e_first,) = pick(density, e_plane, [(0, TILE)], 52)
    first_halo = lax.ppermute(e_first, "py", EVEN_CUTS)
    e, e_rest = pick(density, e_plane, [(0, rows), (TILE, rows)], 50)
    e_halo = lax.ppermute(e_rest, "py", EVEN_CUTS)
    spans = [(0, rows), (0, EARLY), (EARLY, DIRECT), (DIRECT, rows)]
    o, early, late, rest = pick(density, o_plane, spans, 46)
    mid = density
    rows, depth, _ = o.shape
    x_low, x_high = density[:, 0], density[:, rows - 1]
    z_low, z_high = (lax.dynamic_slice_in_dim(density[:, :, k], odd, 3, 0) for k in (0, depth - 1))
    z_even, z_odd = jnp.where(pz_odd == 1, z_low, z_high), jnp.where(pz_odd == 1, z_high, z_low)
    up = [(k, k + 1) for k in range(3)]
    down = [(b, a) for a, b in up]
    half = rows // 2
    for step in range(STEPS):
        z_by = lax.ppermute(z_odd[:, half:], "pz", [(1, 3), (2, 0)])
        z_even = lax.ppermute(z_even, "pz", [(0, 1), (1, 0), (2, 3), (3, 2)])
        z_odd = lax.ppermute(z_odd[:, :half], "pz", [(1, 2), (2, 1)])
        z_by = lax.ppermute(z_by, "pz", [(3, 2), (0, 1)])
        relayed = []
        for to, _ in RELAYS:
            relayed.append(lax.ppermute(rest, "py", to))
        px = [lax.ppermute(x_high, "px", up), lax.ppermute(x_low, "px", down)]
        o_early = lax.ppermute(early, "py", ODD_CUTS)
        for k, (_, on) in enumerate(RELAYS):
            relayed[k] = lax.ppermute(relayed[k], "py", on)
        if step == 0:
            e_halo = jnp.concatenate([first_halo, e_halo])
        low, high = columns(e_halo)
        low, high = lax.ppermute(high, ("py", "pz"), CORNERS_UP), lax.ppermute(low, ("py", "pz"), CORNERS_DOWN)
        o_halos = [o_early, lax.ppermute(late, "py", ODD_CUTS)]
        ends = [*px, z_even, z_odd, z_by]
        o_part, e_part, mid, *mids = partial_step(step, odd_ref, o, mid, e, inverse, ends)
        if step == STEPS - 1:
            break
        e, ex = finish_even(e_part, e_halo, low, high)
        e_halo = lax.ppermute(e, "py", EVEN_CUTS)
        outs = finish_odd(odd_ref, o_part, o_halos, relayed, mids, ex)
        o, early, late, rest, x_low, x_high, z_even, z_odd = outs
    out = place(e_plane, e_part, (e_halo, low, high), mid)
    return place(o_plane, o_part, (*o_halos, *relayed), out)


def solution(mesh):
    spec = P("py", "px", "pz", None)
    return jax.shard_map(local, mesh=mesh, in_specs=(spec, spec), out_specs=spec, check_vma=False)
```

```python
import functools

import jax
import jax.numpy as jnp
from jax import lax
from jax.experimental import pallas as pl
from jax.experimental.pallas import tpu as pltpu
from jax.sharding import PartitionSpec as P


STEPS = 3
ROWS = 8
TILE = 16
EARLY = 16
DIRECT = 48

EVEN_CUTS = [(0, 1), (1, 0), (2, 3), (3, 2), (4, 5), (5, 4), (6, 7), (7, 6)]
ODD_CUTS = [(1, 2), (2, 1), (3, 4), (4, 3), (5, 6), (6, 5)]
RELAYS = [
    ([(6, 0), (1, 7)], [(0, 5), (7, 2)]),
    ([(4, 0), (3, 7)], [(0, 3), (7, 4)]),
    ([(2, 0), (5, 7)], [(0, 1), (7, 6)]),
]
CORNERS_UP = [(4 * a + k, 4 * b + k + 1) for a, b in EVEN_CUTS for k in range(3)]
CORNERS_DOWN = [(4 * a + k + 1, 4 * b + k) for a, b in EVEN_CUTS for k in range(3)]
VMEM = 20 * 1024 * 1024
PART_VMEM = 24 * 1024 * 1024


def struct(*shape):
    return jax.ShapeDtypeStruct(shape, jnp.float32)


def fixed(*shape):
    return pl.BlockSpec(shape, lambda i, *_: (0,) * len(shape))


def partial_kernel(first, last, odd_ref, *refs):
    planes = [refs[3 * s : 3 * s + 3] for s in range(4)]
    inverse, px_low, px_high, z_even, z_odd, z_on = refs[12:18]
    part_o, part_e, kept, mx_low, mx_high, mz_even, mz_odd = (refs[18:] + (None,) * 4)[:7]
    i, blocks = pl.program_id(0), pl.num_programs(0)
    odd, pz_odd = odd_ref[0], odd_ref[1] == 1
    shape = px_low.shape[1:]
    depth = shape[0]
    z = lax.broadcasted_iota(jnp.int32, shape, 0)

    def stored(s):
        return jnp.where(odd == 1, 3 - s, s)

    def edge(s):
        return stored(s) if first else s

    def z_edge(s):
        return stored(s) - odd if first else s

    def main(s, r):
        ref = planes[s][0]
        return ref[r] if len(ref.shape) == 3 else ref[0, r]

    def one_row(r, before, after):
        for s in range(4):
            c = main(s, r)
            if s < 3:
                over_even, over_odd, over_on = (v[z_edge(s), pl.ds(r, 1), :] for v in (z_even, z_odd, z_on))
                over_odd = jnp.where(2 * i < blocks, over_odd, over_on)
                low, high = jnp.where(pz_odd, over_even, over_odd), jnp.where(pz_odd, over_odd, over_even)
            else:
                low = high = 0.0
            below = jnp.where(z == 0, low, pltpu.roll(c, 1, 0))
            above = jnp.where(z == depth - 1, high, pltpu.roll(c, depth - 1, 0))
            total = (before(s) + after(s)) + (below + above)
            if s > 0:
                total = total + main(s - 1, r)
            if s < 3:
                total = total + main(s + 1, r)
            value = c * (0.6 - 0.2 * c * inverse[stored(s), r]) + 0.1 * total
            if s == 0:
                part_o[r] = value
            elif s == 3:
                part_e[r] = value
            elif last:
                kept[stored(s), r] = value
            else:
                kept[s - 1, r] = value
                low, high = value[0:1, :], value[depth - 1 : depth, :]
                mz_even[s - 1, pl.ds(r, 1), :] = jnp.where(pz_odd, low, high)
                mz_odd[s - 1, pl.ds(r, 1), :] = jnp.where(pz_odd, high, low)

    def earlier(s):
        return jnp.where(i == 0, px_low[edge(s)], planes[s][1][...].reshape(shape))

    def later(s):
        return jnp.where(i == blocks - 1, px_high[edge(s)], planes[s][2][...].reshape(shape))

    one_row(0, earlier, lambda s: main(s, 1))

    @pl.loop(1, ROWS - 1)
    def _(r):
        one_row(r, lambda s: main(s, r - 1), lambda s: main(s, r + 1))

    one_row(ROWS - 1, lambda s: main(s, ROWS - 2), later)
    if not last:

        @pl.when(i == 0)
        def _():
            mx_low[...] = kept[:, 0]

        @pl.when(i == blocks - 1)
        def _():
            mx_high[...] = kept[:, ROWS - 1]


def partial_step(step, odd, o, mid, e, inverse, halo_ends):
    first, last = step == 0, step == STEPS - 1
    rows, depth, levels = o.shape

    def specs(plane):
        if plane is None:
            shape, at = (lambda k: (k, depth, levels)), (lambda j, odd_ref: (j, 0, 0))
        else:
            shape, at = (lambda k: (1, k, depth, levels)), (lambda j, odd_ref: (plane(odd_ref), j, 0, 0))
        return [
            pl.BlockSpec(shape(ROWS), lambda i, odd_ref: at(i, odd_ref)),
            pl.BlockSpec(shape(1), lambda i, odd_ref: at(jnp.maximum(i * ROWS - 1, 0), odd_ref)),
            pl.BlockSpec(shape(1), lambda i, odd_ref: at(jnp.minimum(i * ROWS + ROWS, rows - 1), odd_ref)),
        ]

    def middle(s):
        if first:
            return lambda odd_ref: jnp.where(odd_ref[0] == 1, 3 - s, s)
        return lambda odd_ref: s - 1

    def block(planes):
        return pl.BlockSpec((planes, ROWS, depth, levels), lambda i, odd_ref: (0, i, 0, 0))

    def ends(planes):
        return pl.BlockSpec((planes, ROWS, levels), lambda i, odd_ref: (0, i, 0))

    half = rows // ROWS // 2
    half_ends = [
        pl.BlockSpec((3, ROWS, levels), lambda i, odd_ref: (0, jnp.minimum(i, half - 1), 0)),
        pl.BlockSpec((3, ROWS, levels), lambda i, odd_ref: (0, jnp.maximum(i - half, 0), 0)),
    ]
    face = pl.BlockSpec((ROWS, depth, levels), lambda i, odd_ref: (i, 0, 0))
    out_specs = [face, face, block(4 if last else 2)]
    out_shape = [struct(*o.shape), struct(*o.shape), struct(4 if last else 2, *o.shape)]
    if not last:
        out_specs += [fixed(2, depth, levels)] * 2 + [ends(2)] * 2
        out_shape += [struct(2, depth, levels)] * 2 + [struct(2, rows, levels)] * 2
    return pl.pallas_call(
        functools.partial(partial_kernel, first, last),
        grid_spec=pltpu.PrefetchScalarGridSpec(
            num_scalar_prefetch=1,
            grid=(rows // ROWS,),
            in_specs=specs(None)
            + specs(middle(1))
            + specs(middle(2))
            + specs(None)
            + [block(4), fixed(4, depth, levels), fixed(4, depth, levels), ends(3), *half_ends],
            out_specs=out_specs,
        ),
        out_shape=out_shape,
        compiler_params=pltpu.CompilerParams(vmem_limit_bytes=PART_VMEM),
        cost_estimate=pl.CostEstimate(flops=60_000_000, bytes_accessed=40_000_000, transcendentals=0),
        name="partial_step",
    )(odd, *([o] * 3), *([mid] * 6), *([e] * 3), inverse, *halo_ends)


def z_ends_of(odd_ref, face):
    low, high = face[:, 0, :], face[:, face.shape[1] - 1, :]
    pz_odd = odd_ref[1] == 1
    return jnp.where(pz_odd, low, high), jnp.where(pz_odd, high, low)


def finish_even_kernel(part, halo, low, high, face, x_ends):
    i, blocks = pl.program_id(0), pl.num_programs(0)
    depth = face.shape[1]
    face[...] = part[...] + 0.1 * halo[...]
    face[:, 0, :] = face[:, 0, :] + 0.1 * low[...]
    face[:, depth - 1, :] = face[:, depth - 1, :] + 0.1 * high[...]

    @pl.when(i == 0)
    def _():
        x_ends[0] = face[0]

    @pl.when(i == blocks - 1)
    def _():
        x_ends[1] = face[TILE - 1]


def finish_even(part, halo, low, high):
    rows, depth, levels = part.shape
    face = pl.BlockSpec((TILE, depth, levels), lambda i: (i, 0, 0))
    column = pl.BlockSpec((TILE, levels), lambda i: (i, 0))
    return pl.pallas_call(
        finish_even_kernel,
        grid=(rows // TILE,),
        in_specs=[face, face, column, column],
        out_specs=[face, fixed(2, depth, levels)],
        out_shape=[struct(*part.shape), struct(2, depth, levels)],
        compiler_params=pltpu.CompilerParams(vmem_limit_bytes=VMEM),
        cost_estimate=pl.CostEstimate(flops=6_000_000, bytes_accessed=9_500_000, transcendentals=0),
        name="finish_even",
    )(part, halo, low, high)


def columns_kernel(halo, low, high):
    low[...] = halo[:, 0, :]
    high[...] = halo[:, halo.shape[1] - 1, :]


def columns(halo):
    rows, _, levels = halo.shape
    return pl.pallas_call(
        columns_kernel,
        in_specs=[pl.BlockSpec(memory_space=pltpu.VMEM)],
        out_specs=[pl.BlockSpec(memory_space=pltpu.VMEM)] * 2,
        out_shape=[struct(rows, levels)] * 2,
        compiler_params=pltpu.CompilerParams(vmem_limit_bytes=VMEM),
        cost_estimate=pl.CostEstimate(flops=1_000_000, bytes_accessed=100_000, transcendentals=0),
        name="columns",
    )(halo)


def odd_pieces():
    return ((0, EARLY // TILE), (EARLY // TILE, DIRECT // TILE), (DIRECT // TILE, None))


def in_piece(i, piece):
    return i >= piece[0] if piece[1] is None else (i >= piece[0]) & (i < piece[1])


def odd_specs(rows, depth, levels):
    def spec(start, stop):
        last = (rows // TILE if stop is None else stop) - start - 1
        return pl.BlockSpec((TILE, depth, levels), lambda i, *_: (jnp.clip(i - start, 0, last), 0, 0))

    return [spec(*piece) for piece in odd_pieces()]


def finish_odd_kernel(odd_ref, part, early, late, r0, r1, r2, mx_low, mx_high, mz_even, mz_odd, ex, *outs):
    face, *pieces, x_low, x_high, z_even, z_odd = outs
    i, blocks = pl.program_id(0), pl.num_programs(0)

    for (piece, out), halos in zip(zip(odd_pieces(), pieces), ((early,), (late,), (r0, r1, r2))):

        @pl.when(in_piece(i, piece))
        def _(out=out, halos=halos):
            face[...] = part[...] + 0.1 * sum((h[...] for h in halos[1:]), halos[0][...])
            out[...] = face[...]

    z_even[0], z_odd[0] = z_ends_of(odd_ref, face)
    z_even[1:3], z_odd[1:3] = mz_even[...], mz_odd[...]

    @pl.when(i == 0)
    def _():
        x_low[0] = face[0]
        x_low[1:3] = mx_low[...]
        x_low[3] = ex[0]

    @pl.when(i == blocks - 1)
    def _():
        x_high[0] = face[TILE - 1]
        x_high[1:3] = mx_high[...]
        x_high[3] = ex[1]


def finish_odd(odd, part, halos, relayed, mids, ex):
    rows, depth, levels = part.shape
    face = pl.BlockSpec((TILE, depth, levels), lambda i, _: (i, 0, 0))
    early, late, relay = odd_specs(rows, depth, levels)

    def ends(planes):
        return pl.BlockSpec((planes, TILE, levels), lambda i, _: (0, i, 0))

    x2, x4 = fixed(2, depth, levels), fixed(4, depth, levels)
    return pl.pallas_call(
        finish_odd_kernel,
        grid_spec=pltpu.PrefetchScalarGridSpec(
            num_scalar_prefetch=1,
            grid=(rows // TILE,),
            in_specs=[face, early, late, relay, relay, relay, x2, x2, ends(2), ends(2), x2],
            out_specs=[face, early, late, relay, x4, x4, ends(3), ends(3)],
        ),
        out_shape=[struct(*part.shape)]
        + [struct(size, depth, levels) for size in (EARLY, DIRECT - EARLY, rows - DIRECT)]
        + [struct(4, depth, levels)] * 2
        + [struct(3, rows, levels)] * 2,
        compiler_params=pltpu.CompilerParams(vmem_limit_bytes=VMEM),
        cost_estimate=pl.CostEstimate(flops=6_000_000, bytes_accessed=12_600_000, transcendentals=0),
        name="finish_odd",
    )(odd, part, *halos, *relayed, *mids, ex)


def place_kernel(pieces, at_ref, part, *refs):
    halos, (_, out, done, sems) = list(refs[:-4]), refs[-4:]
    plane = out.at[at_ref[0]]
    copies = []
    for start, count in pieces:
        own_halos, halos = halos[:count], halos[count:]
        for at in range(0, own_halos[0].shape[0], TILE):
            rows = pl.ds(at, TILE)
            own = pl.ds(start + at, TILE)
            done[own] = part[own] + 0.1 * sum((h[rows] for h in own_halos[1:]), own_halos[0][rows])
            if len(pieces) == 1 and halos:
                for column, z in zip(halos, (0, part.shape[1] - 1)):
                    done[own, z, :] = done[own, z, :] + 0.1 * column[own]
            copies.append(pltpu.make_async_copy(done.at[own], plane.at[own], sems.at[len(copies)]))
            copies[-1].start()
    for copy in copies:
        copy.wait()


def place(at, part, pieces, edges, whole):
    held = pl.BlockSpec(memory_space=pltpu.VMEM)
    halos = [h for _, some in pieces for h in some] + list(edges)
    return pl.pallas_call(
        functools.partial(place_kernel, [(start, len(some)) for start, some in pieces]),
        in_specs=[pl.BlockSpec(memory_space=pltpu.SMEM), held]
        + [held] * len(halos)
        + [pl.BlockSpec(memory_space=pltpu.HBM)],
        out_specs=pl.BlockSpec(memory_space=pltpu.HBM),
        out_shape=struct(*whole.shape),
        scratch_shapes=[pltpu.VMEM(part.shape, jnp.float32), pltpu.SemaphoreType.DMA((part.shape[0] // TILE,))],
        input_output_aliases={2 + len(halos): 0},
        compiler_params=pltpu.CompilerParams(vmem_limit_bytes=VMEM),
        cost_estimate=pl.CostEstimate(flops=6_000_000, bytes_accessed=9_500_000, transcendentals=0),
        name="place",
    )(at.astype(jnp.int32).reshape(1), part, *halos, whole)


def pick_kernel(starts, at_ref, density, *outs_and_sems):
    outs, sems = outs_and_sems[:-1], outs_and_sems[-1]
    plane = density.at[at_ref[0]]
    copies = [
        pltpu.make_async_copy(plane.at[pl.ds(starts[k], out.shape[0])], out, sems.at[k]) for k, out in enumerate(outs)
    ]
    for copy in copies:
        copy.start()
    for copy in copies:
        copy.wait()


def pick(density, at, spans, grant):
    _, _, depth, levels = density.shape
    return pl.pallas_call(
        functools.partial(pick_kernel, [start for start, _ in spans]),
        in_specs=[pl.BlockSpec(memory_space=pltpu.SMEM), pl.BlockSpec(memory_space=pltpu.HBM)],
        out_specs=[pl.BlockSpec(memory_space=pltpu.VMEM)] * len(spans),
        out_shape=[struct(stop - start, depth, levels) for start, stop in spans],
        scratch_shapes=[pltpu.SemaphoreType.DMA((len(spans),))],
        compiler_params=pltpu.CompilerParams(vmem_limit_bytes=grant * 1024 * 1024),
        cost_estimate=pl.CostEstimate(flops=1_000_000, bytes_accessed=6_300_000, transcendentals=0),
    )(at.astype(jnp.int32).reshape(1), density)


def local(density, inverse):
    odd, pz_odd = lax.axis_index("py") % 2, lax.axis_index("pz") % 2
    odd_ref = jnp.stack([odd, pz_odd]).astype(jnp.int32)
    e_plane, o_plane = 3 * (1 - odd), 3 * odd
    rows = density.shape[1]
    (e_first,) = pick(density, e_plane, [(0, TILE)], 52)
    first_halo = lax.ppermute(e_first, "py", EVEN_CUTS)
    e, e_rest = pick(density, e_plane, [(0, rows), (TILE, rows)], 50)
    e_halo = lax.ppermute(e_rest, "py", EVEN_CUTS)
    spans = [(0, rows), (0, EARLY), (EARLY, DIRECT), (DIRECT, rows)]
    o, early, late, rest = pick(density, o_plane, spans, 46)
    mid = density
    rows, depth, _ = o.shape
    x_low, x_high = density[:, 0], density[:, rows - 1]
    z_low, z_high = (lax.dynamic_slice_in_dim(density[:, :, k], odd, 3, 0) for k in (0, depth - 1))
    z_even, z_odd = jnp.where(pz_odd == 1, z_low, z_high), jnp.where(pz_odd == 1, z_high, z_low)
    up = [(k, k + 1) for k in range(3)]
    down = [(b, a) for a, b in up]
    half = rows // 2
    for step in range(STEPS):
        z_by = lax.ppermute(z_odd[:, half:], "pz", [(1, 3), (2, 0)])
        z_even = lax.ppermute(z_even, "pz", [(0, 1), (1, 0), (2, 3), (3, 2)])
        z_odd = lax.ppermute(z_odd[:, :half], "pz", [(1, 2), (2, 1)])
        z_by = lax.ppermute(z_by, "pz", [(3, 2), (0, 1)])
        relayed = []
        for to, _ in RELAYS:
            relayed.append(lax.ppermute(rest, "py", to))
        px = [lax.ppermute(x_high, "px", up), lax.ppermute(x_low, "px", down)]
        o_early = lax.ppermute(early, "py", ODD_CUTS)
        for k, (_, on) in enumerate(RELAYS):
            relayed[k] = lax.ppermute(relayed[k], "py", on)
        if step == 0:
            e_halo = jnp.concatenate([first_halo, e_halo])
        low, high = columns(e_halo)
        low, high = lax.ppermute(high, ("py", "pz"), CORNERS_UP), lax.ppermute(low, ("py", "pz"), CORNERS_DOWN)
        cut = late.shape[0] if step < STEPS - 1 else late.shape[0] // 2
        o_halos = [o_early, lax.ppermute(late[:cut], "py", ODD_CUTS)]
        o_final = lax.ppermute(late[cut:], "py", ODD_CUTS) if step == STEPS - 1 else None
        ends = [*px, z_even, z_odd, z_by]
        o_part, e_part, mid, *mids = partial_step(step, odd_ref, o, mid, e, inverse, ends)
        if step == STEPS - 1:
            break
        e, ex = finish_even(e_part, e_halo, low, high)
        e_halo = lax.ppermute(e, "py", EVEN_CUTS)
        outs = finish_odd(odd_ref, o_part, o_halos, relayed, mids, ex)
        o, early, late, rest, x_low, x_high, z_even, z_odd = outs
    out = place(e_plane, e_part, [(0, [e_halo])], (low, high), mid)
    out = place(o_plane, o_part, [(0, o_halos[:1]), (EARLY, o_halos[1:])], (), out)
    return place(o_plane, o_part, [(EARLY + cut, [o_final]), (DIRECT, relayed)], (), out)


def solution(mesh):
    spec = P("py", "px", "pz", None)
    return jax.shard_map(local, mesh=mesh, in_specs=(spec, spec), out_specs=spec, check_vma=False)
```

```python
import functools

import jax
import jax.numpy as jnp
from jax import lax
from jax.experimental import pallas as pl
from jax.experimental.pallas import tpu as pltpu
from jax.sharding import PartitionSpec as P


STEPS = 3
ROWS = 8
TILE = 16
EARLY = 16
DIRECT = 48

EVEN_CUTS = [(0, 1), (1, 0), (2, 3), (3, 2), (4, 5), (5, 4), (6, 7), (7, 6)]
ODD_CUTS = [(1, 2), (2, 1), (3, 4), (4, 3), (5, 6), (6, 5)]
RELAYS = [
    ([(6, 0), (1, 7)], [(0, 5), (7, 2)]),
    ([(4, 0), (3, 7)], [(0, 3), (7, 4)]),
    ([(2, 0), (5, 7)], [(0, 1), (7, 6)]),
]
CORNERS_UP = [(4 * a + k, 4 * b + k + 1) for a, b in EVEN_CUTS for k in range(3)]
CORNERS_DOWN = [(4 * a + k + 1, 4 * b + k) for a, b in EVEN_CUTS for k in range(3)]
VMEM = 20 * 1024 * 1024
PART_VMEM = 24 * 1024 * 1024
FIRST_VMEM = 32 * 1024 * 1024


def struct(*shape):
    return jax.ShapeDtypeStruct(shape, jnp.float32)


def fixed(*shape):
    return pl.BlockSpec(shape, lambda i, *_: (0,) * len(shape))


def partial_kernel(first, last, odd_ref, *refs):
    planes = [refs[3 * s : 3 * s + 3] for s in range(4)]
    inverse, px_low, px_high, z_even, z_odd, z_on = refs[12:18]
    part_o, part_e, kept, mx_low, mx_high, mz_even, mz_odd = (refs[18:] + (None,) * 4)[:7]
    i, blocks = pl.program_id(0), pl.num_programs(0)
    odd, pz_odd = odd_ref[0], odd_ref[1] == 1
    shape = px_low.shape[1:]
    depth = shape[0]
    z = lax.broadcasted_iota(jnp.int32, shape, 0)

    def stored(s):
        return jnp.where(odd == 1, 3 - s, s)

    def edge(s):
        return stored(s) if first else s

    def z_edge(s):
        return stored(s) - odd if first else s

    def main(s, r):
        ref = planes[s][0]
        return ref[r] if len(ref.shape) == 3 else ref[0, r]

    def one_row(r, before, after):
        for s in range(4):
            c = main(s, r)
            if s < 3:
                over_even, over_odd, over_on = (v[z_edge(s), pl.ds(r, 1), :] for v in (z_even, z_odd, z_on))
                over_odd = jnp.where(2 * i < blocks, over_odd, over_on)
                low, high = jnp.where(pz_odd, over_even, over_odd), jnp.where(pz_odd, over_odd, over_even)
            else:
                low = high = 0.0
            below = jnp.where(z == 0, low, pltpu.roll(c, 1, 0))
            above = jnp.where(z == depth - 1, high, pltpu.roll(c, depth - 1, 0))
            total = (before(s) + after(s)) + (below + above)
            if s > 0:
                total = total + main(s - 1, r)
            if s < 3:
                total = total + main(s + 1, r)
            value = c * (0.6 - 0.2 * c * inverse[stored(s), r]) + 0.1 * total
            if s == 0:
                part_o[r] = value
            elif s == 3:
                part_e[r] = value
            elif last:
                kept[stored(s), r] = value
            else:
                kept[s - 1, r] = value
                low, high = value[0:1, :], value[depth - 1 : depth, :]
                mz_even[s - 1, pl.ds(r, 1), :] = jnp.where(pz_odd, low, high)
                mz_odd[s - 1, pl.ds(r, 1), :] = jnp.where(pz_odd, high, low)

    def earlier(s):
        return jnp.where(i == 0, px_low[edge(s)], planes[s][1][...].reshape(shape))

    def later(s):
        return jnp.where(i == blocks - 1, px_high[edge(s)], planes[s][2][...].reshape(shape))

    one_row(0, earlier, lambda s: main(s, 1))

    @pl.loop(1, ROWS - 1)
    def _(r):
        one_row(r, lambda s: main(s, r - 1), lambda s: main(s, r + 1))

    one_row(ROWS - 1, lambda s: main(s, ROWS - 2), later)
    if not last:

        @pl.when(i == 0)
        def _():
            mx_low[...] = kept[:, 0]

        @pl.when(i == blocks - 1)
        def _():
            mx_high[...] = kept[:, ROWS - 1]


def partial_step(step, odd, o, mid, e, inverse, halo_ends):
    first, last = step == 0, step == STEPS - 1
    rows, depth, levels = mid.shape[1:]

    def specs(plane):
        if plane is None:
            shape, at = (lambda k: (k, depth, levels)), (lambda j, odd_ref: (j, 0, 0))
        else:
            shape, at = (lambda k: (1, k, depth, levels)), (lambda j, odd_ref: (plane(odd_ref), j, 0, 0))
        return [
            pl.BlockSpec(shape(ROWS), lambda i, odd_ref: at(i, odd_ref)),
            pl.BlockSpec(shape(1), lambda i, odd_ref: at(jnp.maximum(i * ROWS - 1, 0), odd_ref)),
            pl.BlockSpec(shape(1), lambda i, odd_ref: at(jnp.minimum(i * ROWS + ROWS, rows - 1), odd_ref)),
        ]

    def middle(s):
        if first:
            return lambda odd_ref: jnp.where(odd_ref[0] == 1, 3 - s, s)
        return lambda odd_ref: s - 1

    def block(planes):
        return pl.BlockSpec((planes, ROWS, depth, levels), lambda i, odd_ref: (0, i, 0, 0))

    def ends(planes):
        return pl.BlockSpec((planes, ROWS, levels), lambda i, odd_ref: (0, i, 0))

    half = rows // ROWS // 2
    half_ends = [
        pl.BlockSpec((3, ROWS, levels), lambda i, odd_ref: (0, jnp.minimum(i, half - 1), 0)),
        pl.BlockSpec((3, ROWS, levels), lambda i, odd_ref: (0, jnp.maximum(i - half, 0), 0)),
    ]
    face = pl.BlockSpec((ROWS, depth, levels), lambda i, odd_ref: (i, 0, 0))
    out_specs = [face, face, block(4 if last else 2)]
    out_shape = [struct(rows, depth, levels)] * 2 + [struct(4 if last else 2, rows, depth, levels)]
    if not last:
        out_specs += [fixed(2, depth, levels)] * 2 + [ends(2)] * 2
        out_shape += [struct(2, depth, levels)] * 2 + [struct(2, rows, levels)] * 2
    return pl.pallas_call(
        functools.partial(partial_kernel, first, last),
        grid_spec=pltpu.PrefetchScalarGridSpec(
            num_scalar_prefetch=1,
            grid=(rows // ROWS,),
            in_specs=specs(middle(0) if first else None)
            + specs(middle(1))
            + specs(middle(2))
            + specs(middle(3) if first else None)
            + [block(4), fixed(4, depth, levels), fixed(4, depth, levels), ends(3), *half_ends],
            out_specs=out_specs,
        ),
        out_shape=out_shape,
        compiler_params=pltpu.CompilerParams(vmem_limit_bytes=FIRST_VMEM if first else PART_VMEM),
        cost_estimate=pl.CostEstimate(flops=60_000_000, bytes_accessed=40_000_000, transcendentals=0),
        name="partial_step",
    )(odd, *([o] * 3), *([mid] * 6), *([e] * 3), inverse, *halo_ends)


def z_ends_of(odd_ref, face):
    low, high = face[:, 0, :], face[:, face.shape[1] - 1, :]
    pz_odd = odd_ref[1] == 1
    return jnp.where(pz_odd, low, high), jnp.where(pz_odd, high, low)


def finish_even_kernel(part, halo, low, high, face, x_ends):
    i, blocks = pl.program_id(0), pl.num_programs(0)
    depth = face.shape[1]
    face[...] = part[...] + 0.1 * halo[...]
    face[:, 0, :] = face[:, 0, :] + 0.1 * low[...]
    face[:, depth - 1, :] = face[:, depth - 1, :] + 0.1 * high[...]

    @pl.when(i == 0)
    def _():
        x_ends[0] = face[0]

    @pl.when(i == blocks - 1)
    def _():
        x_ends[1] = face[TILE - 1]


def finish_even(part, halo, low, high):
    rows, depth, levels = part.shape
    face = pl.BlockSpec((TILE, depth, levels), lambda i: (i, 0, 0))
    column = pl.BlockSpec((TILE, levels), lambda i: (i, 0))
    return pl.pallas_call(
        finish_even_kernel,
        grid=(rows // TILE,),
        in_specs=[face, face, column, column],
        out_specs=[face, fixed(2, depth, levels)],
        out_shape=[struct(*part.shape), struct(2, depth, levels)],
        compiler_params=pltpu.CompilerParams(vmem_limit_bytes=VMEM),
        cost_estimate=pl.CostEstimate(flops=6_000_000, bytes_accessed=9_500_000, transcendentals=0),
        name="finish_even",
    )(part, halo, low, high)


def columns_kernel(halo, low, high):
    low[...] = halo[:, 0, :]
    high[...] = halo[:, halo.shape[1] - 1, :]


def columns(halo):
    rows, _, levels = halo.shape
    return pl.pallas_call(
        columns_kernel,
        in_specs=[pl.BlockSpec(memory_space=pltpu.VMEM)],
        out_specs=[pl.BlockSpec(memory_space=pltpu.VMEM)] * 2,
        out_shape=[struct(rows, levels)] * 2,
        compiler_params=pltpu.CompilerParams(vmem_limit_bytes=VMEM),
        cost_estimate=pl.CostEstimate(flops=1_000_000, bytes_accessed=100_000, transcendentals=0),
        name="columns",
    )(halo)


def odd_pieces():
    return ((0, EARLY // TILE), (EARLY // TILE, DIRECT // TILE), (DIRECT // TILE, None))


def in_piece(i, piece):
    return i >= piece[0] if piece[1] is None else (i >= piece[0]) & (i < piece[1])


def odd_specs(rows, depth, levels):
    def spec(start, stop):
        last = (rows // TILE if stop is None else stop) - start - 1
        return pl.BlockSpec((TILE, depth, levels), lambda i, *_: (jnp.clip(i - start, 0, last), 0, 0))

    return [spec(*piece) for piece in odd_pieces()]


def finish_odd_kernel(odd_ref, part, early, late, r0, r1, r2, mx_low, mx_high, mz_even, mz_odd, ex, *outs):
    face, *pieces, x_low, x_high, z_even, z_odd = outs
    i, blocks = pl.program_id(0), pl.num_programs(0)

    for (piece, out), halos in zip(zip(odd_pieces(), pieces), ((early,), (late,), (r0, r1, r2))):

        @pl.when(in_piece(i, piece))
        def _(out=out, halos=halos):
            face[...] = part[...] + 0.1 * sum((h[...] for h in halos[1:]), halos[0][...])
            out[...] = face[...]

    z_even[0], z_odd[0] = z_ends_of(odd_ref, face)
    z_even[1:3], z_odd[1:3] = mz_even[...], mz_odd[...]

    @pl.when(i == 0)
    def _():
        x_low[0] = face[0]
        x_low[1:3] = mx_low[...]
        x_low[3] = ex[0]

    @pl.when(i == blocks - 1)
    def _():
        x_high[0] = face[TILE - 1]
        x_high[1:3] = mx_high[...]
        x_high[3] = ex[1]


def finish_odd(odd, part, halos, relayed, mids, ex):
    rows, depth, levels = part.shape
    face = pl.BlockSpec((TILE, depth, levels), lambda i, _: (i, 0, 0))
    early, late, relay = odd_specs(rows, depth, levels)

    def ends(planes):
        return pl.BlockSpec((planes, TILE, levels), lambda i, _: (0, i, 0))

    x2, x4 = fixed(2, depth, levels), fixed(4, depth, levels)
    return pl.pallas_call(
        finish_odd_kernel,
        grid_spec=pltpu.PrefetchScalarGridSpec(
            num_scalar_prefetch=1,
            grid=(rows // TILE,),
            in_specs=[face, early, late, relay, relay, relay, x2, x2, ends(2), ends(2), x2],
            out_specs=[face, early, late, relay, x4, x4, ends(3), ends(3)],
        ),
        out_shape=[struct(*part.shape)]
        + [struct(size, depth, levels) for size in (EARLY, DIRECT - EARLY, rows - DIRECT)]
        + [struct(4, depth, levels)] * 2
        + [struct(3, rows, levels)] * 2,
        compiler_params=pltpu.CompilerParams(vmem_limit_bytes=VMEM),
        cost_estimate=pl.CostEstimate(flops=6_000_000, bytes_accessed=12_600_000, transcendentals=0),
        name="finish_odd",
    )(odd, part, *halos, *relayed, *mids, ex)


def place_kernel(pieces, at_ref, part, *refs):
    halos, (_, out, done, sems) = list(refs[:-4]), refs[-4:]
    plane = out.at[at_ref[0]]
    copies = []
    for start, count in pieces:
        own_halos, halos = halos[:count], halos[count:]
        for at in range(0, own_halos[0].shape[0], TILE):
            rows = pl.ds(at, TILE)
            own = pl.ds(start + at, TILE)
            done[own] = part[own] + 0.1 * sum((h[rows] for h in own_halos[1:]), own_halos[0][rows])
            if len(pieces) == 1 and halos:
                for column, z in zip(halos, (0, part.shape[1] - 1)):
                    done[own, z, :] = done[own, z, :] + 0.1 * column[own]
            copies.append(pltpu.make_async_copy(done.at[own], plane.at[own], sems.at[len(copies)]))
            copies[-1].start()
    for copy in copies:
        copy.wait()


def place(at, part, pieces, edges, whole):
    held = pl.BlockSpec(memory_space=pltpu.VMEM)
    halos = [h for _, some in pieces for h in some] + list(edges)
    return pl.pallas_call(
        functools.partial(place_kernel, [(start, len(some)) for start, some in pieces]),
        in_specs=[pl.BlockSpec(memory_space=pltpu.SMEM), held]
        + [held] * len(halos)
        + [pl.BlockSpec(memory_space=pltpu.HBM)],
        out_specs=pl.BlockSpec(memory_space=pltpu.HBM),
        out_shape=struct(*whole.shape),
        scratch_shapes=[pltpu.VMEM(part.shape, jnp.float32), pltpu.SemaphoreType.DMA((part.shape[0] // TILE,))],
        input_output_aliases={2 + len(halos): 0},
        compiler_params=pltpu.CompilerParams(vmem_limit_bytes=VMEM),
        cost_estimate=pl.CostEstimate(flops=6_000_000, bytes_accessed=9_500_000, transcendentals=0),
        name="place",
    )(at.astype(jnp.int32).reshape(1), part, *halos, whole)


def pick_kernel(starts, at_ref, density, *outs_and_sems):
    outs, sems = outs_and_sems[:-1], outs_and_sems[-1]
    plane = density.at[at_ref[0]]
    copies = [
        pltpu.make_async_copy(plane.at[pl.ds(starts[k], out.shape[0])], out, sems.at[k]) for k, out in enumerate(outs)
    ]
    for copy in copies:
        copy.start()
    for copy in copies:
        copy.wait()


def pick(density, at, spans, grant):
    _, _, depth, levels = density.shape
    return pl.pallas_call(
        functools.partial(pick_kernel, [start for start, _ in spans]),
        in_specs=[pl.BlockSpec(memory_space=pltpu.SMEM), pl.BlockSpec(memory_space=pltpu.HBM)],
        out_specs=[pl.BlockSpec(memory_space=pltpu.VMEM)] * len(spans),
        out_shape=[struct(stop - start, depth, levels) for start, stop in spans],
        scratch_shapes=[pltpu.SemaphoreType.DMA((len(spans),))],
        compiler_params=pltpu.CompilerParams(vmem_limit_bytes=grant * 1024 * 1024),
        cost_estimate=pl.CostEstimate(flops=1_000_000, bytes_accessed=6_300_000, transcendentals=0),
    )(at.astype(jnp.int32).reshape(1), density)


def local(density, inverse):
    odd, pz_odd = lax.axis_index("py") % 2, lax.axis_index("pz") % 2
    odd_ref = jnp.stack([odd, pz_odd]).astype(jnp.int32)
    e_plane, o_plane = 3 * (1 - odd), 3 * odd
    rows = density.shape[1]
    (e_first,) = pick(density, e_plane, [(0, TILE)], 52)
    first_halo = lax.ppermute(e_first, "py", EVEN_CUTS)
    (e_rest,) = pick(density, e_plane, [(TILE, rows)], 50)
    e_halo = lax.ppermute(e_rest, "py", EVEN_CUTS)
    spans = [(0, EARLY), (EARLY, DIRECT), (DIRECT, rows)]
    early, late, rest = pick(density, o_plane, spans, 46)
    o = mid = e = density
    depth = density.shape[2]
    x_low, x_high = density[:, 0], density[:, rows - 1]
    z_low, z_high = (lax.dynamic_slice_in_dim(density[:, :, k], odd, 3, 0) for k in (0, depth - 1))
    z_even, z_odd = jnp.where(pz_odd == 1, z_low, z_high), jnp.where(pz_odd == 1, z_high, z_low)
    up = [(k, k + 1) for k in range(3)]
    down = [(b, a) for a, b in up]
    half = rows // 2
    for step in range(STEPS):
        z_by = lax.ppermute(z_odd[:, half:], "pz", [(1, 3), (2, 0)])
        z_even = lax.ppermute(z_even, "pz", [(0, 1), (1, 0), (2, 3), (3, 2)])
        z_odd = lax.ppermute(z_odd[:, :half], "pz", [(1, 2), (2, 1)])
        z_by = lax.ppermute(z_by, "pz", [(3, 2), (0, 1)])
        relayed = []
        for to, _ in RELAYS:
            relayed.append(lax.ppermute(rest, "py", to))
        px = [lax.ppermute(x_high, "px", up), lax.ppermute(x_low, "px", down)]
        o_early = lax.ppermute(early, "py", ODD_CUTS)
        for k, (_, on) in enumerate(RELAYS):
            relayed[k] = lax.ppermute(relayed[k], "py", on)
        if step == 0:
            e_halo = jnp.concatenate([first_halo, e_halo])
        low, high = columns(e_halo)
        low, high = lax.ppermute(high, ("py", "pz"), CORNERS_UP), lax.ppermute(low, ("py", "pz"), CORNERS_DOWN)
        cut = late.shape[0] if step < STEPS - 1 else late.shape[0] // 2
        o_halos = [o_early, lax.ppermute(late[:cut], "py", ODD_CUTS)]
        o_final = lax.ppermute(late[cut:], "py", ODD_CUTS) if step == STEPS - 1 else None
        ends = [*px, z_even, z_odd, z_by]
        o_part, e_part, mid, *mids = partial_step(step, odd_ref, o, mid, e, inverse, ends)
        if step == STEPS - 1:
            break
        e, ex = finish_even(e_part, e_halo, low, high)
        e_halo = lax.ppermute(e, "py", EVEN_CUTS)
        outs = finish_odd(odd_ref, o_part, o_halos, relayed, mids, ex)
        o, early, late, rest, x_low, x_high, z_even, z_odd = outs
    out = place(e_plane, e_part, [(0, [e_halo])], (low, high), mid)
    out = place(o_plane, o_part, [(0, o_halos[:1]), (EARLY, o_halos[1:])], (), out)
    return place(o_plane, o_part, [(EARLY + cut, [o_final]), (DIRECT, relayed)], (), out)


def solution(mesh):
    spec = P("py", "px", "pz", None)
    return jax.shard_map(local, mesh=mesh, in_specs=(spec, spec), out_specs=spec, check_vma=False)
```

```python
import functools

import jax
import jax.numpy as jnp
from jax import lax
from jax.experimental import pallas as pl
from jax.experimental.pallas import tpu as pltpu
from jax.sharding import PartitionSpec as P


STEPS = 3
ROWS = 8
TILE = 16
EARLY = 16
DIRECT = 48

EVEN_CUTS = [(0, 1), (1, 0), (2, 3), (3, 2), (4, 5), (5, 4), (6, 7), (7, 6)]
ODD_CUTS = [(1, 2), (2, 1), (3, 4), (4, 3), (5, 6), (6, 5)]
RELAYS = [
    ([(6, 0), (1, 7)], [(0, 5), (7, 2)]),
    ([(4, 0), (3, 7)], [(0, 3), (7, 4)]),
    ([(2, 0), (5, 7)], [(0, 1), (7, 6)]),
]
CORNERS_UP = [(4 * a + k, 4 * b + k + 1) for a, b in EVEN_CUTS for k in range(3)]
CORNERS_DOWN = [(4 * a + k + 1, 4 * b + k) for a, b in EVEN_CUTS for k in range(3)]
VMEM = 20 * 1024 * 1024
PART_VMEM = 24 * 1024 * 1024
FIRST_VMEM = 32 * 1024 * 1024


def struct(*shape):
    return jax.ShapeDtypeStruct(shape, jnp.float32)


def fixed(*shape):
    return pl.BlockSpec(shape, lambda i, *_: (0,) * len(shape))


def partial_kernel(first, last, odd_ref, *refs):
    planes = [refs[3 * s : 3 * s + 3] for s in range(4)]
    inverse, px_low, px_high, z_even, z_odd, z_on = refs[12:18]
    part_o, part_e, kept, mx_low, mx_high, mz_even, mz_odd = (refs[18:] + (None,) * 4)[:7]
    i, blocks = pl.program_id(0), pl.num_programs(0)
    odd, pz_odd = odd_ref[0], odd_ref[1] == 1
    shape = px_low.shape[1:]
    depth = shape[0]
    z = lax.broadcasted_iota(jnp.int32, shape, 0)

    def stored(s):
        return jnp.where(odd == 1, 3 - s, s)

    def edge(s):
        return stored(s) if first else s

    def z_edge(s):
        return stored(s) - odd if first else s

    def main(s, r):
        ref = planes[s][0]
        return ref[r] if len(ref.shape) == 3 else ref[0, r]

    def one_row(r, before, after):
        for s in range(4):
            c = main(s, r)
            if s < 3:
                over_even, over_odd, over_on = (v[z_edge(s), pl.ds(r, 1), :] for v in (z_even, z_odd, z_on))
                over_odd = jnp.where(2 * i < blocks, over_odd, over_on)
                low, high = jnp.where(pz_odd, over_even, over_odd), jnp.where(pz_odd, over_odd, over_even)
            else:
                low = high = 0.0
            below = jnp.where(z == 0, low, pltpu.roll(c, 1, 0))
            above = jnp.where(z == depth - 1, high, pltpu.roll(c, depth - 1, 0))
            total = (before(s) + after(s)) + (below + above)
            if s > 0:
                total = total + main(s - 1, r)
            if s < 3:
                total = total + main(s + 1, r)
            value = c * (0.6 - 0.2 * c * inverse[stored(s), r]) + 0.1 * total
            if s == 0:
                part_o[r] = value
            elif s == 3:
                part_e[r] = value
            elif last:
                kept[stored(s), r] = value
            else:
                kept[s - 1, r] = value
                low, high = value[0:1, :], value[depth - 1 : depth, :]
                mz_even[s - 1, pl.ds(r, 1), :] = jnp.where(pz_odd, low, high)
                mz_odd[s - 1, pl.ds(r, 1), :] = jnp.where(pz_odd, high, low)

    def earlier(s):
        return jnp.where(i == 0, px_low[edge(s)], planes[s][1][...].reshape(shape))

    def later(s):
        return jnp.where(i == blocks - 1, px_high[edge(s)], planes[s][2][...].reshape(shape))

    one_row(0, earlier, lambda s: main(s, 1))

    @pl.loop(1, ROWS - 1)
    def _(r):
        one_row(r, lambda s: main(s, r - 1), lambda s: main(s, r + 1))

    one_row(ROWS - 1, lambda s: main(s, ROWS - 2), later)
    if not last:

        @pl.when(i == 0)
        def _():
            mx_low[...] = kept[:, 0]

        @pl.when(i == blocks - 1)
        def _():
            mx_high[...] = kept[:, ROWS - 1]


def partial_step(step, odd, o, mid, e, inverse, halo_ends):
    first, last = step == 0, step == STEPS - 1
    rows, depth, levels = mid.shape[1:]

    def specs(plane):
        if plane is None:
            shape, at = (lambda k: (k, depth, levels)), (lambda j, odd_ref: (j, 0, 0))
        else:
            shape, at = (lambda k: (1, k, depth, levels)), (lambda j, odd_ref: (plane(odd_ref), j, 0, 0))
        return [
            pl.BlockSpec(shape(ROWS), lambda i, odd_ref: at(i, odd_ref)),
            pl.BlockSpec(shape(1), lambda i, odd_ref: at(jnp.maximum(i * ROWS - 1, 0), odd_ref)),
            pl.BlockSpec(shape(1), lambda i, odd_ref: at(jnp.minimum(i * ROWS + ROWS, rows - 1), odd_ref)),
        ]

    def middle(s):
        if first:
            return lambda odd_ref: jnp.where(odd_ref[0] == 1, 3 - s, s)
        return lambda odd_ref: s - 1

    def block(planes):
        return pl.BlockSpec((planes, ROWS, depth, levels), lambda i, odd_ref: (0, i, 0, 0))

    def ends(planes):
        return pl.BlockSpec((planes, ROWS, levels), lambda i, odd_ref: (0, i, 0))

    half = rows // ROWS // 2
    half_ends = [
        pl.BlockSpec((3, ROWS, levels), lambda i, odd_ref: (0, jnp.minimum(i, half - 1), 0)),
        pl.BlockSpec((3, ROWS, levels), lambda i, odd_ref: (0, jnp.maximum(i - half, 0), 0)),
    ]
    face = pl.BlockSpec((ROWS, depth, levels), lambda i, odd_ref: (i, 0, 0))
    out_specs = [face, face, block(4 if last else 2)]
    out_shape = [struct(rows, depth, levels)] * 2 + [struct(4 if last else 2, rows, depth, levels)]
    if not last:
        out_specs += [fixed(2, depth, levels)] * 2 + [ends(2)] * 2
        out_shape += [struct(2, depth, levels)] * 2 + [struct(2, rows, levels)] * 2
    return pl.pallas_call(
        functools.partial(partial_kernel, first, last),
        grid_spec=pltpu.PrefetchScalarGridSpec(
            num_scalar_prefetch=1,
            grid=(rows // ROWS,),
            in_specs=specs(middle(0) if first else None)
            + specs(middle(1))
            + specs(middle(2))
            + specs(middle(3) if first else None)
            + [block(4), fixed(4, depth, levels), fixed(4, depth, levels), ends(3), *half_ends],
            out_specs=out_specs,
        ),
        out_shape=out_shape,
        compiler_params=pltpu.CompilerParams(vmem_limit_bytes=FIRST_VMEM if first else PART_VMEM),
        cost_estimate=pl.CostEstimate(flops=60_000_000, bytes_accessed=40_000_000, transcendentals=0),
        name="partial_step",
    )(odd, *([o] * 3), *([mid] * 6), *([e] * 3), inverse, *halo_ends)


def z_ends_of(odd_ref, face):
    low, high = face[:, 0, :], face[:, face.shape[1] - 1, :]
    pz_odd = odd_ref[1] == 1
    return jnp.where(pz_odd, low, high), jnp.where(pz_odd, high, low)


def finish_even_kernel(part, halo, low, high, face, x_ends):
    i, blocks = pl.program_id(0), pl.num_programs(0)
    depth = face.shape[1]
    face[...] = part[...] + 0.1 * halo[...]
    face[:, 0, :] = face[:, 0, :] + 0.1 * low[...]
    face[:, depth - 1, :] = face[:, depth - 1, :] + 0.1 * high[...]

    @pl.when(i == 0)
    def _():
        x_ends[0] = face[0]

    @pl.when(i == blocks - 1)
    def _():
        x_ends[1] = face[TILE - 1]


def finish_even(part, halo, low, high):
    rows, depth, levels = part.shape
    face = pl.BlockSpec((TILE, depth, levels), lambda i: (i, 0, 0))
    column = pl.BlockSpec((TILE, levels), lambda i: (i, 0))
    return pl.pallas_call(
        finish_even_kernel,
        grid=(rows // TILE,),
        in_specs=[face, face, column, column],
        out_specs=[face, fixed(2, depth, levels)],
        out_shape=[struct(*part.shape), struct(2, depth, levels)],
        compiler_params=pltpu.CompilerParams(vmem_limit_bytes=VMEM),
        cost_estimate=pl.CostEstimate(flops=6_000_000, bytes_accessed=9_500_000, transcendentals=0),
        name="finish_even",
    )(part, halo, low, high)


def columns_kernel(halo, low, high):
    low[...] = halo[:, 0, :]
    high[...] = halo[:, halo.shape[1] - 1, :]


def columns(halo):
    rows, _, levels = halo.shape
    return pl.pallas_call(
        columns_kernel,
        in_specs=[pl.BlockSpec(memory_space=pltpu.VMEM)],
        out_specs=[pl.BlockSpec(memory_space=pltpu.VMEM)] * 2,
        out_shape=[struct(rows, levels)] * 2,
        compiler_params=pltpu.CompilerParams(vmem_limit_bytes=VMEM),
        cost_estimate=pl.CostEstimate(flops=1_000_000, bytes_accessed=100_000, transcendentals=0),
        name="columns",
    )(halo)


def odd_pieces():
    return ((0, EARLY // TILE), (EARLY // TILE, DIRECT // TILE), (DIRECT // TILE, None))


def in_piece(i, piece):
    return i >= piece[0] if piece[1] is None else (i >= piece[0]) & (i < piece[1])


def odd_specs(rows, depth, levels):
    def spec(start, stop):
        last = (rows // TILE if stop is None else stop) - start - 1
        return pl.BlockSpec((TILE, depth, levels), lambda i, *_: (jnp.clip(i - start, 0, last), 0, 0))

    return [spec(*piece) for piece in odd_pieces()]


def finish_odd_kernel(odd_ref, part, early, late, r0, r1, r2, mx_low, mx_high, mz_even, mz_odd, ex, *outs):
    face, *pieces, x_low, x_high, z_even, z_odd = outs
    i, blocks = pl.program_id(0), pl.num_programs(0)

    for (piece, out), halos in zip(zip(odd_pieces(), pieces), ((early,), (late,), (r0, r1, r2))):

        @pl.when(in_piece(i, piece))
        def _(out=out, halos=halos):
            face[...] = part[...] + 0.1 * sum((h[...] for h in halos[1:]), halos[0][...])
            out[...] = face[...]

    z_even[0], z_odd[0] = z_ends_of(odd_ref, face)
    z_even[1:3], z_odd[1:3] = mz_even[...], mz_odd[...]

    @pl.when(i == 0)
    def _():
        x_low[0] = face[0]
        x_low[1:3] = mx_low[...]
        x_low[3] = ex[0]

    @pl.when(i == blocks - 1)
    def _():
        x_high[0] = face[TILE - 1]
        x_high[1:3] = mx_high[...]
        x_high[3] = ex[1]


def finish_odd(odd, part, halos, relayed, mids, ex):
    rows, depth, levels = part.shape
    face = pl.BlockSpec((TILE, depth, levels), lambda i, _: (i, 0, 0))
    early, late, relay = odd_specs(rows, depth, levels)

    def ends(planes):
        return pl.BlockSpec((planes, TILE, levels), lambda i, _: (0, i, 0))

    x2, x4 = fixed(2, depth, levels), fixed(4, depth, levels)
    return pl.pallas_call(
        finish_odd_kernel,
        grid_spec=pltpu.PrefetchScalarGridSpec(
            num_scalar_prefetch=1,
            grid=(rows // TILE,),
            in_specs=[face, early, late, relay, relay, relay, x2, x2, ends(2), ends(2), x2],
            out_specs=[face, early, late, relay, x4, x4, ends(3), ends(3)],
        ),
        out_shape=[struct(*part.shape)]
        + [struct(size, depth, levels) for size in (EARLY, DIRECT - EARLY, rows - DIRECT)]
        + [struct(4, depth, levels)] * 2
        + [struct(3, rows, levels)] * 2,
        compiler_params=pltpu.CompilerParams(vmem_limit_bytes=VMEM),
        cost_estimate=pl.CostEstimate(flops=6_000_000, bytes_accessed=12_600_000, transcendentals=0),
        name="finish_odd",
    )(odd, part, *halos, *relayed, *mids, ex)


def place_kernel(pieces, at_ref, part, *refs):
    halos, (_, out, done, sems) = list(refs[:-4]), refs[-4:]
    plane = out.at[at_ref[0]]
    copies = []
    for start, count in pieces:
        own_halos, halos = halos[:count], halos[count:]
        for at in range(0, own_halos[0].shape[0], ROWS):
            rows = pl.ds(at, ROWS)
            own = pl.ds(start + at, ROWS)
            done[own] = part[own] + 0.1 * sum((h[rows] for h in own_halos[1:]), own_halos[0][rows])
            if len(pieces) == 1 and halos:
                for column, z in zip(halos, (0, part.shape[1] - 1)):
                    done[own, z, :] = done[own, z, :] + 0.1 * column[own]
            copies.append(pltpu.make_async_copy(done.at[own], plane.at[own], sems.at[len(copies)]))
            copies[-1].start()
    for copy in copies:
        copy.wait()


def place(at, part, pieces, edges, whole):
    held = pl.BlockSpec(memory_space=pltpu.VMEM)
    halos = [h for _, some in pieces for h in some] + list(edges)
    return pl.pallas_call(
        functools.partial(place_kernel, [(start, len(some)) for start, some in pieces]),
        in_specs=[pl.BlockSpec(memory_space=pltpu.SMEM), held]
        + [held] * len(halos)
        + [pl.BlockSpec(memory_space=pltpu.HBM)],
        out_specs=pl.BlockSpec(memory_space=pltpu.HBM),
        out_shape=struct(*whole.shape),
        scratch_shapes=[pltpu.VMEM(part.shape, jnp.float32), pltpu.SemaphoreType.DMA((part.shape[0] // ROWS,))],
        input_output_aliases={2 + len(halos): 0},
        compiler_params=pltpu.CompilerParams(vmem_limit_bytes=VMEM),
        cost_estimate=pl.CostEstimate(flops=6_000_000, bytes_accessed=9_500_000, transcendentals=0),
        name="place",
    )(at.astype(jnp.int32).reshape(1), part, *halos, whole)


def pick_kernel(starts, at_ref, density, *outs_and_sems):
    outs, sems = outs_and_sems[:-1], outs_and_sems[-1]
    plane = density.at[at_ref[0]]
    copies = [
        pltpu.make_async_copy(plane.at[pl.ds(starts[k], out.shape[0])], out, sems.at[k]) for k, out in enumerate(outs)
    ]
    for copy in copies:
        copy.start()
    for copy in copies:
        copy.wait()


def pick(density, at, spans, grant):
    _, _, depth, levels = density.shape
    return pl.pallas_call(
        functools.partial(pick_kernel, [start for start, _ in spans]),
        in_specs=[pl.BlockSpec(memory_space=pltpu.SMEM), pl.BlockSpec(memory_space=pltpu.HBM)],
        out_specs=[pl.BlockSpec(memory_space=pltpu.VMEM)] * len(spans),
        out_shape=[struct(stop - start, depth, levels) for start, stop in spans],
        scratch_shapes=[pltpu.SemaphoreType.DMA((len(spans),))],
        compiler_params=pltpu.CompilerParams(vmem_limit_bytes=grant * 1024 * 1024),
        cost_estimate=pl.CostEstimate(flops=1_000_000, bytes_accessed=6_300_000, transcendentals=0),
    )(at.astype(jnp.int32).reshape(1), density)


def local(density, inverse):
    odd, pz_odd = lax.axis_index("py") % 2, lax.axis_index("pz") % 2
    odd_ref = jnp.stack([odd, pz_odd]).astype(jnp.int32)
    e_plane, o_plane = 3 * (1 - odd), 3 * odd
    rows = density.shape[1]
    (e_first,) = pick(density, e_plane, [(0, TILE)], 52)
    first_halo = lax.ppermute(e_first, "py", EVEN_CUTS)
    (e_rest,) = pick(density, e_plane, [(TILE, rows)], 50)
    e_halo = lax.ppermute(e_rest, "py", EVEN_CUTS)
    spans = [(0, EARLY), (EARLY, DIRECT), (DIRECT, rows)]
    early, late, rest = pick(density, o_plane, spans, 46)
    o = mid = e = density
    depth = density.shape[2]
    x_low, x_high = density[:, 0], density[:, rows - 1]
    z_low, z_high = (lax.dynamic_slice_in_dim(density[:, :, k], odd, 3, 0) for k in (0, depth - 1))
    z_even, z_odd = jnp.where(pz_odd == 1, z_low, z_high), jnp.where(pz_odd == 1, z_high, z_low)
    up = [(k, k + 1) for k in range(3)]
    down = [(b, a) for a, b in up]
    half = rows // 2
    for step in range(STEPS):
        z_by = lax.ppermute(z_odd[:, half:], "pz", [(1, 3), (2, 0)])
        z_even = lax.ppermute(z_even, "pz", [(0, 1), (1, 0), (2, 3), (3, 2)])
        z_odd = lax.ppermute(z_odd[:, :half], "pz", [(1, 2), (2, 1)])
        z_by = lax.ppermute(z_by, "pz", [(3, 2), (0, 1)])
        relayed = []
        for to, _ in RELAYS:
            relayed.append(lax.ppermute(rest, "py", to))
        px = [lax.ppermute(x_high, "px", up), lax.ppermute(x_low, "px", down)]
        o_early = lax.ppermute(early, "py", ODD_CUTS)
        for k, (_, on) in enumerate(RELAYS):
            relayed[k] = lax.ppermute(relayed[k], "py", on)
        if step == 0:
            e_halo = jnp.concatenate([first_halo, e_halo])
        low, high = columns(e_halo)
        low, high = lax.ppermute(high, ("py", "pz"), CORNERS_UP), lax.ppermute(low, ("py", "pz"), CORNERS_DOWN)
        cut = late.shape[0] if step < STEPS - 1 else late.shape[0] - ROWS
        o_halos = [o_early, lax.ppermute(late[:cut], "py", ODD_CUTS)]
        o_final = lax.ppermute(late[cut:], "py", ODD_CUTS) if step == STEPS - 1 else None
        ends = [*px, z_even, z_odd, z_by]
        o_part, e_part, mid, *mids = partial_step(step, odd_ref, o, mid, e, inverse, ends)
        if step == STEPS - 1:
            break
        e, ex = finish_even(e_part, e_halo, low, high)
        e_halo = lax.ppermute(e, "py", EVEN_CUTS)
        outs = finish_odd(odd_ref, o_part, o_halos, relayed, mids, ex)
        o, early, late, rest, x_low, x_high, z_even, z_odd = outs
    out = place(e_plane, e_part, [(0, [e_halo])], (low, high), mid)
    out = place(o_plane, o_part, [(0, o_halos[:1]), (EARLY, o_halos[1:])], (), out)
    return place(o_plane, o_part, [(EARLY + cut, [o_final]), (DIRECT, relayed)], (), out)


def solution(mesh):
    spec = P("py", "px", "pz", None)
    return jax.shard_map(local, mesh=mesh, in_specs=(spec, spec), out_specs=spec, check_vma=False)
```

```python
import functools

import jax
import jax.numpy as jnp
from jax import lax
from jax.experimental import pallas as pl
from jax.experimental.pallas import tpu as pltpu
from jax.sharding import PartitionSpec as P


STEPS = 3
ROWS = 8
TILE = 16
EARLY = 16
DIRECT = 48

EVEN_CUTS = [(0, 1), (1, 0), (2, 3), (3, 2), (4, 5), (5, 4), (6, 7), (7, 6)]
ODD_CUTS = [(1, 2), (2, 1), (3, 4), (4, 3), (5, 6), (6, 5)]
RELAYS = [
    ([(6, 0), (1, 7)], [(0, 5), (7, 2)]),
    ([(4, 0), (3, 7)], [(0, 3), (7, 4)]),
    ([(2, 0), (5, 7)], [(0, 1), (7, 6)]),
]
CORNERS_UP = [(4 * a + k, 4 * b + k + 1) for a, b in EVEN_CUTS for k in range(3)]
CORNERS_DOWN = [(4 * a + k + 1, 4 * b + k) for a, b in EVEN_CUTS for k in range(3)]
VMEM = 20 * 1024 * 1024
PART_VMEM = 24 * 1024 * 1024
FIRST_VMEM = 32 * 1024 * 1024


def struct(*shape):
    return jax.ShapeDtypeStruct(shape, jnp.float32)


def fixed(*shape):
    return pl.BlockSpec(shape, lambda i, *_: (0,) * len(shape))


def partial_kernel(first, last, odd_ref, *refs):
    planes = [refs[3 * s : 3 * s + 3] for s in range(4)]
    inverse, px_low, px_high, z_even, z_odd, z_on = refs[12:18]
    part_o, part_e, kept, mx_low, mx_high, mz_even, mz_odd = (refs[18:] + (None,) * 4)[:7]
    i, blocks = pl.program_id(0), pl.num_programs(0)
    odd, pz_odd = odd_ref[0], odd_ref[1] == 1
    shape = px_low.shape[1:]
    depth = shape[0]
    z = lax.broadcasted_iota(jnp.int32, shape, 0)

    def stored(s):
        return jnp.where(odd == 1, 3 - s, s)

    def edge(s):
        return stored(s) if first else s

    def z_edge(s):
        return stored(s) - odd if first else s

    def main(s, r):
        ref = planes[s][0]
        return ref[r] if len(ref.shape) == 3 else ref[0, r]

    def one_row(r, before, after):
        for s in range(4):
            c = main(s, r)
            if s < 3:
                over_even, over_odd, over_on = (v[z_edge(s), pl.ds(r, 1), :] for v in (z_even, z_odd, z_on))
                over_odd = jnp.where(2 * i < blocks, over_odd, over_on)
                low, high = jnp.where(pz_odd, over_even, over_odd), jnp.where(pz_odd, over_odd, over_even)
            else:
                low = high = 0.0
            below = jnp.where(z == 0, low, pltpu.roll(c, 1, 0))
            above = jnp.where(z == depth - 1, high, pltpu.roll(c, depth - 1, 0))
            total = (before(s) + after(s)) + (below + above)
            if s > 0:
                total = total + main(s - 1, r)
            if s < 3:
                total = total + main(s + 1, r)
            value = c * (0.6 - 0.2 * c * inverse[stored(s), r]) + 0.1 * total
            if s == 0:
                part_o[r] = value
            elif s == 3:
                part_e[r] = value
            elif last:
                kept[stored(s), r] = value
            else:
                kept[s - 1, r] = value
                low, high = value[0:1, :], value[depth - 1 : depth, :]
                mz_even[s - 1, pl.ds(r, 1), :] = jnp.where(pz_odd, low, high)
                mz_odd[s - 1, pl.ds(r, 1), :] = jnp.where(pz_odd, high, low)

    def earlier(s):
        return jnp.where(i == 0, px_low[edge(s)], planes[s][1][...].reshape(shape))

    def later(s):
        return jnp.where(i == blocks - 1, px_high[edge(s)], planes[s][2][...].reshape(shape))

    one_row(0, earlier, lambda s: main(s, 1))

    @pl.loop(1, ROWS - 1)
    def _(r):
        one_row(r, lambda s: main(s, r - 1), lambda s: main(s, r + 1))

    one_row(ROWS - 1, lambda s: main(s, ROWS - 2), later)
    if not last:

        @pl.when(i == 0)
        def _():
            mx_low[...] = kept[:, 0]

        @pl.when(i == blocks - 1)
        def _():
            mx_high[...] = kept[:, ROWS - 1]


def partial_step(step, odd, o, mid, e, inverse, halo_ends):
    first, last = step == 0, step == STEPS - 1
    rows, depth, levels = mid.shape[1:]

    def specs(plane):
        if plane is None:
            shape, at = (lambda k: (k, depth, levels)), (lambda j, odd_ref: (j, 0, 0))
        else:
            shape, at = (lambda k: (1, k, depth, levels)), (lambda j, odd_ref: (plane(odd_ref), j, 0, 0))
        return [
            pl.BlockSpec(shape(ROWS), lambda i, odd_ref: at(i, odd_ref)),
            pl.BlockSpec(shape(1), lambda i, odd_ref: at(jnp.maximum(i * ROWS - 1, 0), odd_ref)),
            pl.BlockSpec(shape(1), lambda i, odd_ref: at(jnp.minimum(i * ROWS + ROWS, rows - 1), odd_ref)),
        ]

    def middle(s):
        if first:
            return lambda odd_ref: jnp.where(odd_ref[0] == 1, 3 - s, s)
        return lambda odd_ref: s - 1

    def block(planes):
        return pl.BlockSpec((planes, ROWS, depth, levels), lambda i, odd_ref: (0, i, 0, 0))

    def ends(planes):
        return pl.BlockSpec((planes, ROWS, levels), lambda i, odd_ref: (0, i, 0))

    half = rows // ROWS // 2
    half_ends = [
        pl.BlockSpec((3, ROWS, levels), lambda i, odd_ref: (0, jnp.minimum(i, half - 1), 0)),
        pl.BlockSpec((3, ROWS, levels), lambda i, odd_ref: (0, jnp.maximum(i - half, 0), 0)),
    ]
    face = pl.BlockSpec((ROWS, depth, levels), lambda i, odd_ref: (i, 0, 0))
    out_specs = [face, face, block(4 if last else 2)]
    out_shape = [struct(rows, depth, levels)] * 2 + [struct(4 if last else 2, rows, depth, levels)]
    if not last:
        out_specs += [fixed(2, depth, levels)] * 2 + [ends(2)] * 2
        out_shape += [struct(2, depth, levels)] * 2 + [struct(2, rows, levels)] * 2
    return pl.pallas_call(
        functools.partial(partial_kernel, first, last),
        grid_spec=pltpu.PrefetchScalarGridSpec(
            num_scalar_prefetch=1,
            grid=(rows // ROWS,),
            in_specs=specs(middle(0) if first else None)
            + specs(middle(1))
            + specs(middle(2))
            + specs(middle(3) if first else None)
            + [block(4), fixed(4, depth, levels), fixed(4, depth, levels), ends(3), *half_ends],
            out_specs=out_specs,
        ),
        out_shape=out_shape,
        compiler_params=pltpu.CompilerParams(vmem_limit_bytes=FIRST_VMEM if first else PART_VMEM),
        cost_estimate=pl.CostEstimate(flops=60_000_000, bytes_accessed=40_000_000, transcendentals=0),
        name="partial_step",
    )(odd, *([o] * 3), *([mid] * 6), *([e] * 3), inverse, *halo_ends)


def z_ends_of(odd_ref, face):
    low, high = face[:, 0, :], face[:, face.shape[1] - 1, :]
    pz_odd = odd_ref[1] == 1
    return jnp.where(pz_odd, low, high), jnp.where(pz_odd, high, low)


def finish_even_kernel(part, halo, low, high, face, x_ends):
    i, blocks = pl.program_id(0), pl.num_programs(0)
    depth = face.shape[1]
    face[...] = part[...] + 0.1 * halo[...]
    face[:, 0, :] = face[:, 0, :] + 0.1 * low[...]
    face[:, depth - 1, :] = face[:, depth - 1, :] + 0.1 * high[...]

    @pl.when(i == 0)
    def _():
        x_ends[0] = face[0]

    @pl.when(i == blocks - 1)
    def _():
        x_ends[1] = face[TILE - 1]


def finish_even(part, halo, low, high):
    rows, depth, levels = part.shape
    face = pl.BlockSpec((TILE, depth, levels), lambda i: (i, 0, 0))
    column = pl.BlockSpec((TILE, levels), lambda i: (i, 0))
    return pl.pallas_call(
        finish_even_kernel,
        grid=(rows // TILE,),
        in_specs=[face, face, column, column],
        out_specs=[face, fixed(2, depth, levels)],
        out_shape=[struct(*part.shape), struct(2, depth, levels)],
        compiler_params=pltpu.CompilerParams(vmem_limit_bytes=VMEM),
        cost_estimate=pl.CostEstimate(flops=6_000_000, bytes_accessed=9_500_000, transcendentals=0),
        name="finish_even",
    )(part, halo, low, high)


def columns_kernel(halo, low, high):
    low[...] = halo[:, 0, :]
    high[...] = halo[:, halo.shape[1] - 1, :]


def columns(halo):
    rows, _, levels = halo.shape
    return pl.pallas_call(
        columns_kernel,
        in_specs=[pl.BlockSpec(memory_space=pltpu.VMEM)],
        out_specs=[pl.BlockSpec(memory_space=pltpu.VMEM)] * 2,
        out_shape=[struct(rows, levels)] * 2,
        compiler_params=pltpu.CompilerParams(vmem_limit_bytes=VMEM),
        cost_estimate=pl.CostEstimate(flops=1_000_000, bytes_accessed=100_000, transcendentals=0),
        name="columns",
    )(halo)


def odd_pieces():
    return ((0, EARLY // TILE), (EARLY // TILE, DIRECT // TILE), (DIRECT // TILE, None))


def in_piece(i, piece):
    return i >= piece[0] if piece[1] is None else (i >= piece[0]) & (i < piece[1])


def odd_specs(rows, depth, levels):
    def spec(start, stop):
        last = (rows // TILE if stop is None else stop) - start - 1
        return pl.BlockSpec((TILE, depth, levels), lambda i, *_: (jnp.clip(i - start, 0, last), 0, 0))

    return [spec(*piece) for piece in odd_pieces()]


def finish_odd_kernel(odd_ref, part, early, late, r0, r1, r2, mx_low, mx_high, mz_even, mz_odd, ex, *outs):
    face, *pieces, x_low, x_high, z_even, z_odd = outs
    i, blocks = pl.program_id(0), pl.num_programs(0)

    for (piece, out), halos in zip(zip(odd_pieces(), pieces), ((early,), (late,), (r0, r1, r2))):

        @pl.when(in_piece(i, piece))
        def _(out=out, halos=halos):
            face[...] = part[...] + 0.1 * sum((h[...] for h in halos[1:]), halos[0][...])
            out[...] = face[...]

    z_even[0], z_odd[0] = z_ends_of(odd_ref, face)
    z_even[1:3], z_odd[1:3] = mz_even[...], mz_odd[...]

    @pl.when(i == 0)
    def _():
        x_low[0] = face[0]
        x_low[1:3] = mx_low[...]
        x_low[3] = ex[0]

    @pl.when(i == blocks - 1)
    def _():
        x_high[0] = face[TILE - 1]
        x_high[1:3] = mx_high[...]
        x_high[3] = ex[1]


def finish_odd(odd, part, halos, relayed, mids, ex):
    rows, depth, levels = part.shape
    face = pl.BlockSpec((TILE, depth, levels), lambda i, _: (i, 0, 0))
    early, late, relay = odd_specs(rows, depth, levels)

    def ends(planes):
        return pl.BlockSpec((planes, TILE, levels), lambda i, _: (0, i, 0))

    x2, x4 = fixed(2, depth, levels), fixed(4, depth, levels)
    return pl.pallas_call(
        finish_odd_kernel,
        grid_spec=pltpu.PrefetchScalarGridSpec(
            num_scalar_prefetch=1,
            grid=(rows // TILE,),
            in_specs=[face, early, late, relay, relay, relay, x2, x2, ends(2), ends(2), x2],
            out_specs=[face, early, late, relay, x4, x4, ends(3), ends(3)],
        ),
        out_shape=[struct(*part.shape)]
        + [struct(size, depth, levels) for size in (EARLY, DIRECT - EARLY, rows - DIRECT)]
        + [struct(4, depth, levels)] * 2
        + [struct(3, rows, levels)] * 2,
        compiler_params=pltpu.CompilerParams(vmem_limit_bytes=VMEM),
        cost_estimate=pl.CostEstimate(flops=6_000_000, bytes_accessed=12_600_000, transcendentals=0),
        name="finish_odd",
    )(odd, part, *halos, *relayed, *mids, ex)


def place_kernel(pieces, at_ref, part, *refs):
    halos, (_, out, done, sems) = list(refs[:-4]), refs[-4:]
    plane = out.at[at_ref[0]]
    copies = []
    for start, count in pieces:
        own_halos, halos = halos[:count], halos[count:]
        for at in range(0, own_halos[0].shape[0], ROWS):
            rows = pl.ds(at, ROWS)
            own = pl.ds(start + at, ROWS)
            done[own] = part[own] + 0.1 * sum((h[rows] for h in own_halos[1:]), own_halos[0][rows])
            if len(pieces) == 1 and halos:
                for column, z in zip(halos, (0, part.shape[1] - 1)):
                    done[own, z, :] = done[own, z, :] + 0.1 * column[own]
            copies.append(pltpu.make_async_copy(done.at[own], plane.at[own], sems.at[len(copies)]))
            copies[-1].start()
    for copy in copies:
        copy.wait()


def place(at, part, pieces, edges, whole):
    held = pl.BlockSpec(memory_space=pltpu.VMEM)
    halos = [h for _, some in pieces for h in some] + list(edges)
    return pl.pallas_call(
        functools.partial(place_kernel, [(start, len(some)) for start, some in pieces]),
        in_specs=[pl.BlockSpec(memory_space=pltpu.SMEM), held]
        + [held] * len(halos)
        + [pl.BlockSpec(memory_space=pltpu.HBM)],
        out_specs=pl.BlockSpec(memory_space=pltpu.HBM),
        out_shape=struct(*whole.shape),
        scratch_shapes=[pltpu.VMEM(part.shape, jnp.float32), pltpu.SemaphoreType.DMA((part.shape[0] // ROWS,))],
        input_output_aliases={2 + len(halos): 0},
        compiler_params=pltpu.CompilerParams(vmem_limit_bytes=VMEM),
        cost_estimate=pl.CostEstimate(flops=6_000_000, bytes_accessed=9_500_000, transcendentals=0),
        name="place",
    )(at.astype(jnp.int32).reshape(1), part, *halos, whole)


def pick_kernel(starts, at_ref, density, *outs_and_sems):
    outs, sems = outs_and_sems[:-1], outs_and_sems[-1]
    plane = density.at[at_ref[0]]
    copies = [
        pltpu.make_async_copy(plane.at[pl.ds(starts[k], out.shape[0])], out, sems.at[k]) for k, out in enumerate(outs)
    ]
    for copy in copies:
        copy.start()
    for copy in copies:
        copy.wait()


def pick(density, at, spans, grant):
    _, _, depth, levels = density.shape
    return pl.pallas_call(
        functools.partial(pick_kernel, [start for start, _ in spans]),
        in_specs=[pl.BlockSpec(memory_space=pltpu.SMEM), pl.BlockSpec(memory_space=pltpu.HBM)],
        out_specs=[pl.BlockSpec(memory_space=pltpu.VMEM)] * len(spans),
        out_shape=[struct(stop - start, depth, levels) for start, stop in spans],
        scratch_shapes=[pltpu.SemaphoreType.DMA((len(spans),))],
        compiler_params=pltpu.CompilerParams(vmem_limit_bytes=grant * 1024 * 1024),
        cost_estimate=pl.CostEstimate(flops=1_000_000, bytes_accessed=6_300_000, transcendentals=0),
    )(at.astype(jnp.int32).reshape(1), density)


def local(density, inverse):
    odd, pz_odd = lax.axis_index("py") % 2, lax.axis_index("pz") % 2
    odd_ref = jnp.stack([odd, pz_odd]).astype(jnp.int32)
    e_plane, o_plane = 3 * (1 - odd), 3 * odd
    rows = density.shape[1]
    (e_first,) = pick(density, e_plane, [(0, ROWS)], 52)
    first_halo = lax.ppermute(e_first, "py", EVEN_CUTS)
    (e_rest,) = pick(density, e_plane, [(ROWS, rows)], 50)
    e_halo = lax.ppermute(e_rest, "py", EVEN_CUTS)
    spans = [(0, EARLY), (EARLY, DIRECT), (DIRECT, rows)]
    early, late, rest = pick(density, o_plane, spans, 46)
    o = mid = e = density
    depth = density.shape[2]
    x_low, x_high = density[:, 0], density[:, rows - 1]
    z_low, z_high = (lax.dynamic_slice_in_dim(density[:, :, k], odd, 3, 0) for k in (0, depth - 1))
    z_even, z_odd = jnp.where(pz_odd == 1, z_low, z_high), jnp.where(pz_odd == 1, z_high, z_low)
    up = [(k, k + 1) for k in range(3)]
    down = [(b, a) for a, b in up]
    half = rows // 2
    for step in range(STEPS):
        z_by = lax.ppermute(z_odd[:, half:], "pz", [(1, 3), (2, 0)])
        z_even = lax.ppermute(z_even, "pz", [(0, 1), (1, 0), (2, 3), (3, 2)])
        z_odd = lax.ppermute(z_odd[:, :half], "pz", [(1, 2), (2, 1)])
        z_by = lax.ppermute(z_by, "pz", [(3, 2), (0, 1)])
        relayed = []
        for to, _ in RELAYS:
            relayed.append(lax.ppermute(rest, "py", to))
        px = [lax.ppermute(x_high, "px", up), lax.ppermute(x_low, "px", down)]
        o_early = lax.ppermute(early, "py", ODD_CUTS)
        for k, (_, on) in enumerate(RELAYS):
            relayed[k] = lax.ppermute(relayed[k], "py", on)
        if step == 0:
            e_halo = jnp.concatenate([first_halo, e_halo])
        low, high = columns(e_halo)
        low, high = lax.ppermute(high, ("py", "pz"), CORNERS_UP), lax.ppermute(low, ("py", "pz"), CORNERS_DOWN)
        cut = late.shape[0] if step < STEPS - 1 else late.shape[0] - ROWS
        o_halos = [o_early, lax.ppermute(late[:cut], "py", ODD_CUTS)]
        o_final = lax.ppermute(late[cut:], "py", ODD_CUTS) if step == STEPS - 1 else None
        ends = [*px, z_even, z_odd, z_by]
        o_part, e_part, mid, *mids = partial_step(step, odd_ref, o, mid, e, inverse, ends)
        if step == STEPS - 1:
            break
        e, ex = finish_even(e_part, e_halo, low, high)
        e_halo = lax.ppermute(e, "py", EVEN_CUTS)
        outs = finish_odd(odd_ref, o_part, o_halos, relayed, mids, ex)
        o, early, late, rest, x_low, x_high, z_even, z_odd = outs
    out = place(e_plane, e_part, [(0, [e_halo])], (low, high), mid)
    out = place(o_plane, o_part, [(0, o_halos[:1]), (EARLY, o_halos[1:])], (), out)
    out = place(o_plane, o_part, [(DIRECT, relayed)], (), out)
    return place(o_plane, o_part, [(EARLY + cut, [o_final])], (), out)


def solution(mesh):
    spec = P("py", "px", "pz", None)
    return jax.shard_map(local, mesh=mesh, in_specs=(spec, spec), out_specs=spec, check_vma=False)
```
